128 devices in a mesh: dp: 32 (over y, x, core), tp: 4 (over z).
Axes of the slice: x: 4, y: 4, z: 4, core: 2. Of those that a mesh axis runs over, the one named last changes fastest.
Arguments:
- tokens: bfloat16 [16384, 4096], P(('dp', 'tp')), may hold values from -6 to 6
- norm_gain: float32 [4096], replicated, may hold values from 0.1 to 1.9
- w_query: bfloat16 [4096, 4096], P(None, 'tp'), may hold values from -0.09375 to 0.09375
- w_key: bfloat16 [4096, 1024], P(None, 'tp'), may hold values from -2.34375 to 2.34375
- w_value: bfloat16 [4096, 1024], P(None, 'tp'), may hold values from -0.09375 to 0.09375
- w_output: bfloat16 [4096, 4096], P('tp'), may hold values from -0.09375 to 0.09375
- doc_lengths: int32 [128], replicated, may hold values from 1 to 512, as said below
- pack_index: int32 [16384], replicated, may hold values from 0 to 16383, as said below
Outputs:
- output: bfloat16 [16384, 4096], P(('dp', 'tp'))
The draws below stay inside these ranges and needn't reach their ends.
Inputs may be any that keep to these rules, and one draw needn't show every extreme that they name: `doc_lengths`: each run of 4 documents numbered g * 4 to g * 4 + 4 - 1 (the documents of group g) holds at most 1024 tokens together, and some group holds exactly 1024. No document is longer than 512 tokens, and one has exactly that many. `pack_index`: each packed position appears once. The 128 rows of one device hold at most 8 tokens of the documents of any one group; every device holds the same number of one group's tokens, up to one.
All inputs are finite; a program needn't handle non-finite values.
Results may differ from the reference program's by a relative error of at most 0.01.
Values may be sent and summed in bfloat16 or wider, within the bound.
A program may use at most 128 MiB of HBM per device.

```python
import jax
import jax.numpy as jnp
from jax import lax

D = 4096
HEADS = 32
KV_HEADS = 8
HEAD_DIM = 128
TOK_DEV = 128
GROUP_DOCS = 4
TOKENS = 16384
DOCS = 128
CAP = 1024
N_DP = 32
DEVICES = 128


def query_columns(key):
    return jax.random.truncated_normal(jax.random.fold_in(key, 11), -6.0, 6.0, (D, HEADS * HEAD_DIM), jnp.float32) * D ** (-0.5)


def draw_w_query(key, part):
    return query_columns(key).astype(jnp.bfloat16)


def draw_w_key(key, part):
    own_draw = jax.random.truncated_normal(jax.random.fold_in(key, 13), -6.0, 6.0, (D, KV_HEADS * HEAD_DIM), jnp.float32) * D ** (-0.5)
    return own_draw.astype(jnp.bfloat16)


def layout_plan(key):
    root_random_key = jax.random.fold_in(key, 29)
    complete_random_key, split_random_key, reward_random_key, jitter_random_key, permute_random_key, turning_random_key = jax.random.split(root_random_key, 6)
    full_group = jax.random.randint(complete_random_key, (), 0, N_DP).astype(jnp.int32)
    half_cap = CAP // 2
    cut_points = jnp.sort(jax.random.permutation(split_random_key, half_cap - 1)[:GROUP_DOCS - 2] + 1).astype(jnp.int32)
    fences = jnp.concatenate([jnp.zeros((1,), jnp.int32), cut_points, jnp.full((1,), half_cap, jnp.int32)])
    lesser_lengths = fences[1:] - fences[:-1]
    unrolled = jnp.concatenate([jnp.full((1,), half_cap, jnp.int32), lesser_lengths])
    turning = jax.random.randint(turning_random_key, (), 0, GROUP_DOCS).astype(jnp.int32)
    full_lengths = jnp.roll(unrolled, turning).astype(jnp.int32)
    remaining_documents = (N_DP - 1) * GROUP_DOCS
    spare_capacity = CAP // GROUP_DOCS - 1
    extra_total = TOKENS - CAP - remaining_documents
    extra_reward = jax.random.randint(reward_random_key, (remaining_documents, 1), 0, 4).astype(jnp.int32)
    random_jitter = jax.random.randint(jitter_random_key, (remaining_documents, spare_capacity), 0, 1024).astype(jnp.int32)
    score_values = (extra_reward * 300 + random_jitter) * (remaining_documents * spare_capacity) + jnp.arange(remaining_documents * spare_capacity, dtype=jnp.int32).reshape(remaining_documents, spare_capacity)
    chosen = lax.top_k(score_values.reshape(-1), extra_total)[1].astype(jnp.int32)
    other_lengths = 1 + jax.ops.segment_sum(jnp.ones_like(chosen), chosen // spare_capacity, remaining_documents).astype(jnp.int32)
    slots = jnp.arange(DOCS, dtype=jnp.int32)
    slot_group = slots // GROUP_DOCS
    other_place = jnp.clip(slots - GROUP_DOCS * (slot_group > full_group).astype(jnp.int32), 0, remaining_documents - 1)
    lengths = jnp.where(slot_group == full_group, full_lengths[slots % GROUP_DOCS], other_lengths[other_place]).astype(jnp.int32)
    doc_ends = jnp.cumsum(lengths).astype(jnp.int32)
    doc_starts = doc_ends - lengths
    dealing = jnp.arange(TOKENS, dtype=jnp.int32)
    inside = ((dealing[:, None] >= doc_starts[None, :]) & (dealing[:, None] < doc_ends[None, :])).astype(jnp.int32)
    which_doc = jnp.sum(inside * jnp.arange(DOCS, dtype=jnp.int32)[None, :], axis=1)
    offset = dealing - jnp.sum(inside * doc_starts[None, :], axis=1)
    packed = doc_starts[which_doc] + offset
    dealt = packed.reshape(TOK_DEV, DEVICES).T
    shuffle = jnp.argsort(jax.random.randint(permute_random_key, (DEVICES, TOK_DEV), 0, 1 << 20).astype(jnp.int32) * TOK_DEV + jnp.arange(TOK_DEV, dtype=jnp.int32)[None, :], axis=1)
    placed = jnp.take_along_axis(dealt, shuffle, axis=1).reshape(TOKENS).astype(jnp.int32)
    return (lengths, placed)


def draw_doc_lengths(key, part):
    return layout_plan(key)[0]


def draw_pack_index(key, part):
    return layout_plan(key)[1]


def shard_levels(key, shape, pieces, low, largest):
    def one(axis_at, shards_of):
        heights = jax.random.uniform(jax.random.fold_in(jax.random.fold_in(key, 6), axis_at), (shards_of,), jnp.float32, low / len(pieces), largest / len(pieces))
        return jnp.repeat(jnp.exp(heights), shape[axis_at] // shards_of).reshape((-1,) + (1,) * (len(shape) - axis_at - 1))

    loudness = one(*pieces[0])
    for cut in pieces[1:]:
        loudness = loudness * one(*cut)
    return loudness


def bell_draw(rng, dims, width, bound, cuts=(), held_as=jnp.bfloat16):
    drawn = jax.random.normal(rng, dims, jnp.float32) * width
    if len(cuts) > 0:
        drawn = shard_levels(rng, dims, cuts, -0.22, 0.18) * drawn
    return jnp.clip(drawn, min=-bound, max=bound).astype(held_as)


def setup_inputs(seed: int = 0) -> dict:
    keys = jax.random.split(jax.random.key(seed), 9)
    return {
        "tokens": bell_draw(keys[0], (TOKENS, D), 1.0, 6.0, ((0, 128),)),
        "norm_gain": jnp.clip(1.0 + 0.18 * jax.random.normal(keys[1], (D,), jnp.float32), 0.1, 1.9),
        "w_query": draw_w_query(jax.random.fold_in(keys[8], 71), 0),
        "w_key": draw_w_key(jax.random.fold_in(keys[8], 71), 0),
        "w_value": bell_draw(keys[4], (D, KV_HEADS * HEAD_DIM), D ** -0.5, 0.09375, ((1, 4),)),
        "w_output": bell_draw(keys[5], (HEADS * HEAD_DIM, D), (HEADS * HEAD_DIM) ** -0.5, 0.09375, ((0, 4),)),
        "doc_lengths": draw_doc_lengths(jax.random.fold_in(keys[8], 71), 0),
        "pack_index": draw_pack_index(jax.random.fold_in(keys[8], 71), 0),
    }


rope_base = 500000.0
norm_eps = 1e-05
score_floor = -1e+30

def row_facts(pack_index, doc_lengths):
    doc_ends = jnp.cumsum(doc_lengths).astype(jnp.int32)
    doc_starts = doc_ends - doc_lengths
    inside = ((pack_index[:, None] >= doc_starts[None, :]) & (pack_index[:, None] < doc_ends[None, :])).astype(jnp.int32)
    doc_index = lax.optimization_barrier(jnp.sum(inside * jnp.arange(doc_lengths.shape[0], dtype=jnp.int32)[None, :], axis=1))
    position = pack_index - lax.optimization_barrier(jnp.sum(inside * doc_starts[None, :], axis=1))
    owner_group = (doc_index // GROUP_DOCS).astype(jnp.int32)
    return (doc_index, position, owner_group)

def rotate(projected, position, head_count):
    row_count = projected.shape[0]
    half_dim = HEAD_DIM // 2
    spread = projected.reshape(row_count, head_count, HEAD_DIM)
    frequency = rope_base ** (-2.0 * jnp.arange(half_dim, dtype=jnp.float32) / HEAD_DIM)
    angles = position.astype(jnp.float32)[:, None] * frequency[None, :]
    cosine = jnp.cos(angles)[:, None, :]
    sine = jnp.sin(angles)[:, None, :]
    lower_part = spread[:, :, :half_dim]
    upper_part = spread[:, :, half_dim:]
    turned = jnp.concatenate([lower_part * cosine - upper_part * sine, upper_part * cosine + lower_part * sine], axis=2)
    return turned.reshape(row_count, head_count * HEAD_DIM)

def attend_exact(query, key_rows, value_rows, segment, places):
    slot_total = query.shape[0]
    group_size = HEADS // KV_HEADS
    query_heads = query.astype(jnp.float32).reshape(slot_total, KV_HEADS, group_size, HEAD_DIM)
    key_heads = key_rows.astype(jnp.float32).reshape(slot_total, KV_HEADS, HEAD_DIM)
    value_heads = value_rows.astype(jnp.float32).reshape(slot_total, KV_HEADS, HEAD_DIM)
    score_values = jnp.einsum('qkgd,skd->kgqs', query_heads, key_heads, precision=lax.Precision.HIGHEST) * HEAD_DIM ** (-0.5)
    allowed = (segment[:, None] == segment[None, :]) & (places[None, :] <= places[:, None])
    score_values = jnp.where(allowed[None, None], score_values, score_floor)
    row_peak = lax.optimization_barrier(jnp.max(score_values, axis=-1, keepdims=True))
    weights = jnp.exp(score_values - row_peak)
    weights = (weights / lax.optimization_barrier(jnp.sum(weights, axis=-1, keepdims=True))).astype(jnp.bfloat16)
    mixed_values = jnp.einsum('kgqs,skd->qkgd', weights.astype(jnp.float32), value_heads, precision=lax.Precision.HIGHEST)
    return mixed_values.astype(jnp.bfloat16).reshape(slot_total, HEADS * HEAD_DIM)

def reference(tokens, norm_gain, w_query, w_key, w_value, w_output, doc_lengths, pack_index):
    doc_index, position, owner_group = row_facts(pack_index, doc_lengths)
    residual = tokens.astype(jnp.float32)
    normed = (residual * lax.rsqrt(lax.optimization_barrier(jnp.mean(residual * residual, axis=1, keepdims=True)) + norm_eps) * norm_gain).astype(jnp.bfloat16)
    query = rotate(jnp.dot(normed, w_query, preferred_element_type=jnp.float32), position, HEADS).astype(jnp.bfloat16)
    key_rows = rotate(jnp.dot(normed, w_key, preferred_element_type=jnp.float32), position, KV_HEADS).astype(jnp.bfloat16)
    value_rows = jnp.dot(normed, w_value, preferred_element_type=jnp.float32).astype(jnp.bfloat16)
    ranked = jnp.argsort(owner_group * TOKENS + jnp.arange(TOKENS, dtype=jnp.int32)).astype(jnp.int32)
    counts = jax.ops.segment_sum(jnp.ones((TOKENS,), jnp.int32), owner_group, N_DP).astype(jnp.int32)
    firsts = (jnp.cumsum(counts) - counts).astype(jnp.int32)
    padded = jnp.concatenate([ranked, jnp.zeros((CAP,), jnp.int32)])
    slot_ids = jnp.arange(CAP, dtype=jnp.int32)

    def one_group(gathered, group_id):
        chosen = lax.dynamic_slice_in_dim(padded, firsts[group_id], CAP)
        occupied = slot_ids < counts[group_id]
        segment = jnp.where(occupied, doc_index[chosen], -1 - slot_ids)
        places = jnp.where(occupied, position[chosen], 0)
        context = attend_exact(query[chosen], key_rows[chosen], value_rows[chosen], segment, places)
        target = jnp.where(occupied, chosen, TOKENS)
        return (gathered.at[target].set(context, mode='drop'), None)
    gathered, _ = lax.scan(one_group, jnp.zeros((TOKENS, HEADS * HEAD_DIM), jnp.bfloat16), jnp.arange(N_DP, dtype=jnp.int32))
    attended = jnp.dot(gathered, w_output, preferred_element_type=jnp.float32)
    return (residual + attended).astype(jnp.bfloat16)
```

```python
import functools
import math

import jax
import jax.numpy as jnp
from jax import lax
from jax.experimental import pallas as pl
from jax.experimental.pallas import tpu as pltpu
from jax.sharding import PartitionSpec as P

HEAD_DIM = 128
GROUP_DOCS = 4
SLOTS = 8
rope_base = 500000.0
norm_eps = 1e-05
score_floor = -1e30
MESH = pl.DeviceIdType.MESH
F32 = jnp.float32
BF16 = jnp.bfloat16


def iota(shape, dim):
    return lax.broadcasted_iota(jnp.int32, shape, dim)


def kernel(
    x_ref, gain_ref, pidx_ref, len_ref, wq_ref, wk_ref, wv_ref, wo_ref, out_ref,
    w_all, w_out, gathered, scaled, acc, sumsq, stacked, sent, arrived, qkv,
    slot_row, slot_col, slot_start, bias, unpack, mixed, back_sent, back, unpacked,
    part, half_a, half_b, from_left, from_right, own_part,
    w_sem, wo_sem, ag_send, ag_recv, send_sem, recv_sem, back_send, back_recv, rs_send, rs_recv,
):
    groups = lax.axis_size("dp")
    rows, width = x_ref.shape
    piece = width // 4
    half = width // 2
    docs = len_ref.shape[1]
    me = lax.axis_index("dp")
    z = lax.axis_index("tp")
    right = lax.rem(z + 1, 4)
    left = lax.rem(z + 3, 4)
    members = (z, left, right, lax.rem(z + 2, 4))
    q_cols = wq_ref.shape[1]
    k_cols = wk_ref.shape[1]
    heads = q_cols // HEAD_DIM
    kv_heads = k_cols // HEAD_DIM
    per_kv = heads // kv_heads
    side = (per_kv + 2) * HEAD_DIM
    ctx = per_kv * HEAD_DIM
    pack_rows = 2 * SLOTS
    nb = min(16, groups)
    chunk_slots = SLOTS * groups

    def cols(k):
        return pl.ds(k * piece, piece) if isinstance(k, int) else pl.ds(pl.multiple_of(k * piece, 128), piece)

    def w_copies(k):
        at = cols(k)
        return (
            pltpu.make_async_copy(wq_ref.at[at, :], w_all.at[at, pl.ds(0, q_cols)], w_sem.at[0, k]),
            pltpu.make_async_copy(wk_ref.at[at, :], w_all.at[at, pl.ds(q_cols, k_cols)], w_sem.at[1, k]),
            pltpu.make_async_copy(wv_ref.at[at, :], w_all.at[at, pl.ds(q_cols + k_cols, k_cols)], w_sem.at[2, k]),
        )

    for k in range(4):
        for copy in w_copies(k):
            copy.start()
    wo_copy = pltpu.make_async_copy(wo_ref, w_out, wo_sem)
    wo_copy.start()

    barrier = pltpu.get_barrier_semaphore()

    def greet(i, carry):
        pl.semaphore_signal(barrier, inc=1, device_id=(lax.rem(me + i, groups), z), device_id_type=MESH)
        return carry

    for neighbour in (right, left):
        pl.semaphore_signal(barrier, inc=1, device_id=(me, neighbour), device_id_type=MESH)
    lax.fori_loop(1, groups, greet, 0)
    pl.semaphore_wait(barrier, groups + 1)

    def column_copy(src, dst, send, recv, to):
        return pltpu.make_async_remote_copy(
            src_ref=src, dst_ref=dst, send_sem=send, recv_sem=recv, device_id=(me, to), device_id_type=MESH
        )

    def own_right(k):
        return column_copy(x_ref.at[:, cols(k)], gathered.at[0, :, cols(k)], ag_send.at[0, k], ag_recv.at[0, k], right)

    def own_left(k):
        return column_copy(x_ref.at[:, cols(k)], gathered.at[1, :, cols(k)], ag_send.at[1, k], ag_recv.at[1, k], left)

    def forward(k):
        source, to = (0, right) if k < 2 else (1, left)
        return column_copy(
            gathered.at[source, :, cols(k)], gathered.at[2, :, cols(k)], ag_send.at[2, k], ag_recv.at[2, k], to
        )

    for k in range(4):
        own_right(k).start()
        own_left((k + 2) % 4).start()

    lane = iota((1, docs), 1)
    lens_row = len_ref[...].astype(F32)
    eye_docs = iota((docs, docs), 0) == iota((docs, docs), 1)
    lens_col = jnp.sum(jnp.where(eye_docs, lens_row, 0.0), axis=1, keepdims=True)
    before = iota((docs, docs), 0) < iota((docs, docs), 1)
    starts_row = jnp.sum(jnp.where(before, lens_col, 0.0), axis=0, keepdims=True)
    group_of = iota((groups, docs), 0)
    lane_g = iota((groups, docs), 1)
    group_lo = jnp.sum(jnp.where(lane_g < GROUP_DOCS * group_of, lens_row, 0.0), axis=1, keepdims=True)
    group_hi = jnp.sum(jnp.where(lane_g < GROUP_DOCS * (group_of + 1), lens_row, 0.0), axis=1, keepdims=True)

    def upto(count):
        return jnp.sum(jnp.where(lane < count, lens_row, 0.0), axis=1, keepdims=True)

    my_lo = upto(GROUP_DOCS * me)
    my_hi = upto(GROUP_DOCS * (me + 1))
    my_starts = [upto(GROUP_DOCS * me + i) - my_lo for i in range(1, GROUP_DOCS)]
    earlier = (iota((rows, rows), 0) < iota((rows, rows), 1)).astype(BF16)
    spread_p = (iota((pack_rows * groups, groups), 0) // pack_rows == iota((pack_rows * groups, groups), 1)).astype(BF16)
    spread_s = (iota((chunk_slots, groups), 0) // SLOTS == iota((chunk_slots, groups), 1)).astype(BF16)

    def dot(a, b):
        return jnp.dot(a, b, preferred_element_type=F32)

    def slot_tables(c):
        index = pidx_ref[members[c], :, :].astype(F32)
        mine = (index >= my_lo) & (index < my_hi)
        rank = dot(jnp.where(mine, 1.0, 0.0).astype(BF16), earlier)
        code = jnp.where(mine, rank, -1.0).astype(BF16)
        place = jnp.where(mine, index - my_lo, 0.0)
        high = jnp.floor(place * (1.0 / 32.0))
        low = place - high * 32.0
        code_s = dot(spread_s, code)
        place_s = dot(spread_s, high.astype(BF16)) * 32.0 + dot(spread_s, low.astype(BF16))
        wanted = (iota((chunk_slots, rows), 0) % SLOTS).astype(F32)
        found = jnp.sum(jnp.where(code_s == wanted, place_s + 1.0, 0.0), axis=1, keepdims=True) - 1.0
        begin = jnp.zeros_like(found)
        for start in my_starts:
            begin = jnp.where(found >= start, start, begin)
        slot_col[c] = jnp.broadcast_to(found, (chunk_slots, 128))
        slot_start[c] = jnp.broadcast_to(begin, (chunk_slots, 128))
        same = iota((chunk_slots, chunk_slots), 0) == iota((chunk_slots, chunk_slots), 1)
        slot_row[:, pl.ds(c * chunk_slots, chunk_slots)] = jnp.sum(jnp.where(same, found, 0.0), axis=0, keepdims=True)

    sumsq[...] = jnp.zeros_like(sumsq)
    acc[...] = jnp.zeros_like(acc)
    total_cols = q_cols + 2 * k_cols
    n_tile = 512

    def project(c, k):
        at = cols(k)
        x = (x_ref[:, at] if c == 0 else gathered[c - 1, :, at]).astype(F32)
        squares = sumsq[c]
        for j in range(piece // 128):
            block = x[:, j * 128 : (j + 1) * 128]
            squares = squares + block * block
        sumsq[c] = squares
        scaled[...] = (x * gain_ref[:, at]).astype(BF16)
        for n in range(total_cols // n_tile):
            to = pl.ds(n * n_tile, n_tile)
            acc[c, :, to] += dot(scaled[...], w_all[at, to])

    def dispatch(c):
        scale = lax.rsqrt(jnp.sum(sumsq[c], axis=1, keepdims=True) * (1.0 / width) + norm_eps)
        index = pidx_ref[members[c], pl.ds(me, 1), :].astype(F32)
        eye = iota((rows, rows), 0) == iota((rows, rows), 1)
        index_col = jnp.sum(jnp.where(eye, index, 0.0), axis=1, keepdims=True)
        begin = jnp.max(jnp.where(starts_row <= index_col, starts_row, 0.0), axis=1, keepdims=True)
        place = index_col - begin
        lanes = iota((1, HEAD_DIM), 1)
        exponent = (lanes % (HEAD_DIM // 2)).astype(F32) * (-2.0 * math.log(rope_base) / HEAD_DIM)
        angle = place * jnp.exp(exponent)
        cosine = jnp.cos(angle)
        sine = jnp.where(lanes < HEAD_DIM // 2, -1.0, 1.0) * jnp.sin(angle)

        def head(column):
            return acc[c, :, pl.ds(column * HEAD_DIM, HEAD_DIM)] * scale

        def rope(t):
            return t * cosine + pltpu.roll(t, HEAD_DIM // 2, 1) * sine

        for g in range(kv_heads):
            at = pl.ds(g * rows, rows)
            for j in range(per_kv):
                stacked[at, pl.ds(j * HEAD_DIM, HEAD_DIM)] = rope(head(g * per_kv + j)).astype(BF16)
            stacked[at, pl.ds(ctx, HEAD_DIM)] = rope(head(heads + g)).astype(BF16)
            stacked[at, pl.ds(ctx + HEAD_DIM, HEAD_DIM)] = head(heads + kv_heads + g).astype(BF16)

        inside = (index >= group_lo) & (index < group_hi)
        rank = dot(jnp.where(inside, 1.0, 0.0).astype(BF16), earlier)
        code = jnp.where(inside, rank, -100.0).astype(BF16)
        spread = dot(spread_p, code)
        wanted = (iota((pack_rows * groups, rows), 0) % pack_rows).astype(F32)
        pick = [jnp.where(spread + float(SLOTS * g) == wanted, 1.0, 0.0) for g in range(2)]
        for g in range(2):
            unpack[c, pl.ds(g * rows, rows), :] = jnp.transpose(pick[g]).astype(BF16)
        pick = jnp.concatenate(pick, axis=1).astype(BF16)
        for b in range(groups // nb):
            block = pick[b * nb * pack_rows : (b + 1) * nb * pack_rows]
            sent[pl.ds(c * groups + b * nb, nb)] = (
                dot(block, stacked[...]).astype(BF16).reshape(nb, pack_rows, side)
            )
        arrived[c * groups + me] = sent[c * groups + me]

        def send(i, carry):
            to = lax.rem(me + i, groups)
            pltpu.make_async_remote_copy(
                src_ref=sent.at[c * groups + to],
                dst_ref=arrived.at[c * groups + me],
                send_sem=send_sem.at[c],
                recv_sem=recv_sem.at[c],
                device_id=(to, z),
                device_id_type=MESH,
            ).start()
            return carry

        lax.fori_loop(1, groups, send, 0)

    def all_but_one(ref, c, sem):
        block = ref.at[pl.ds(c * groups, groups - 1)]
        pltpu.make_async_copy(block, block, sem.at[c]).wait()

    reorder_rows = pack_rows * nb
    out_row = iota((reorder_rows, reorder_rows), 0)
    in_row = iota((reorder_rows, reorder_rows), 1)
    split = nb * SLOTS
    source_row = (out_row % split) // SLOTS * pack_rows + out_row // split * SLOTS + out_row % SLOTS
    apart = (source_row == in_row).astype(BF16)
    source_back = (in_row % split) // SLOTS * pack_rows + in_row // split * SLOTS + in_row % SLOTS
    together = (source_back == out_row).astype(BF16)

    def receive(c):
        all_but_one(arrived, c, recv_sem)
        for b in range(groups // nb):
            block = arrived[pl.ds(c * groups + b * nb, nb)].reshape(reorder_rows, side)
            ordered = dot(apart, block).astype(BF16)
            for g in range(2):
                qkv[g, pl.ds(c * chunk_slots + b * split, split), :] = ordered[g * split : (g + 1) * split]

    def attend(c):
        found = slot_col[c][:, :1]
        begin = slot_start[c][:, :1]
        keys = slot_row[...]
        bias[...] = jnp.where((keys >= begin) & (keys <= found), 0.0, score_floor)
        at = pl.ds(c * chunk_slots, chunk_slots)

        def one_head(i, carry):
            g = i // per_kv
            lanes = pl.ds(pl.multiple_of(i % per_kv * HEAD_DIM, HEAD_DIM), HEAD_DIM)
            query = qkv[g, at, lanes]
            key = qkv[g, :, pl.ds(ctx, HEAD_DIM)]
            value = qkv[g, :, pl.ds(ctx + HEAD_DIM, HEAD_DIM)]
            scores = lax.dot_general(query, key, (((1,), (1,)), ((), ())), preferred_element_type=F32)
            scores = scores * HEAD_DIM ** (-0.5) + bias[...]
            weights = jnp.exp(scores - jnp.max(scores, axis=1, keepdims=True))
            total = jnp.sum(weights, axis=1, keepdims=True)
            mixed[g, :, lanes] = (dot(weights.astype(BF16), value) / total).astype(BF16)
            return carry

        lax.fori_loop(0, heads, one_head, 0)
        for b in range(groups // nb):
            block = mixed[:, pl.ds(b * split, split), :].reshape(reorder_rows, ctx)
            back_sent[pl.ds(c * groups + b * nb, nb)] = dot(together, block).astype(BF16).reshape(nb, pack_rows, ctx)
        back[c * groups + me] = back_sent[c * groups + me]

        def send(i, carry):
            to = lax.rem(me + i, groups)
            pltpu.make_async_remote_copy(
                src_ref=back_sent.at[c * groups + to],
                dst_ref=back.at[c * groups + me],
                send_sem=back_send.at[c],
                recv_sem=back_recv.at[c],
                device_id=(to, z),
                device_id_type=MESH,
            ).start()
            return carry

        lax.fori_loop(1, groups, send, 0)

    o_tile = min(512, half)
    per_half = half // o_tile

    def fetch(c):
        all_but_one(back, c, back_recv)
        block = back[pl.ds(c * groups, groups)].reshape(pack_rows * groups, ctx)
        both = dot(unpack[c], block).astype(BF16)
        for g in range(2):
            unpacked[:, pl.ds(g * ctx, ctx)] = both[g * rows : (g + 1) * rows]

    def tile(n):
        return pl.ds(pl.multiple_of(n * o_tile, 128), o_tile)

    def output_half(c, which, extra):
        def step(n, carry):
            at = tile(which * per_half + n)
            value = dot(unpacked[...], w_out[:, at])
            if extra is not None:
                value = value + extra[:, tile(n)].astype(F32)
            part[c - 1, :, at] = value.astype(BF16)
            return carry

        lax.fori_loop(0, per_half, step, 0)

    halves = (pl.ds(0, half), pl.ds(half, half))
    sums = {
        "a": lambda: column_copy(part.at[2, :, halves[0]], half_a, rs_send.at[0], rs_recv.at[0], right),
        "b": lambda: column_copy(part.at[2, :, halves[1]], half_b, rs_send.at[1], rs_recv.at[1], left),
        "r0": lambda: column_copy(part.at[1, :, halves[0]], from_left.at[:, halves[0]], rs_send.at[2], rs_recv.at[2], right),
        "r1": lambda: column_copy(part.at[1, :, halves[1]], from_left.at[:, halves[1]], rs_send.at[3], rs_recv.at[3], right),
        "l0": lambda: column_copy(part.at[0, :, halves[0]], from_right.at[:, halves[0]], rs_send.at[4], rs_recv.at[4], left),
        "l1": lambda: column_copy(part.at[0, :, halves[1]], from_right.at[:, halves[1]], rs_send.at[5], rs_recv.at[5], left),
    }

    with jax.named_scope("own_chunk"):
        for k in range(4):
            for copy in w_copies(k):
                copy.wait()
            project(0, k)
        dispatch(0)
    with jax.named_scope("tables"):
        for c in range(4):
            slot_tables(c)
    with jax.named_scope("neighbour_chunks"):
        for j in range(4):
            k, m = j, (j + 2) % 4
            own_right(k).wait_recv()
            if k < 2:
                forward(k).start()
            own_left(m).wait_recv()
            if m >= 2:
                forward(m).start()
            project(1, k)
            project(2, m)
        dispatch(1)
        dispatch(2)
    receive(0)
    with jax.named_scope("far_chunk"):
        for k in (0, 2, 1, 3):
            forward(k).wait_recv()
            project(3, k)
        dispatch(3)
    for c in range(1, 4):
        receive(c)
    wo_copy.wait()
    with jax.named_scope("attend"):
        attend(3)
        attend(2)
        fetch(3)
        output_half(3, 0, None)
        sums["a"]().start()
        output_half(3, 1, None)
        sums["b"]().start()
        attend(1)
        fetch(2)
        output_half(2, 1, None)
        sums["r1"]().start()
        sums["a"]().wait_recv()
        output_half(2, 0, half_a)
        sums["r0"]().start()
        attend(0)
        fetch(1)
        output_half(1, 0, None)
        sums["l0"]().start()
        sums["b"]().wait_recv()
        output_half(1, 1, half_b)
        sums["l1"]().start()
        fetch(0)

    def own_step(n, carry):
        at = tile(n)
        own_part[:, at] = x_ref[:, at].astype(F32) + dot(unpacked[...], w_out[:, at])
        return carry

    lax.fori_loop(0, 2 * per_half, own_step, 0)

    def finish(which):
        def step(n, carry):
            at = tile(which * per_half + n)
            out_ref[:, at] = (
                own_part[:, at] + from_left[:, at].astype(F32) + from_right[:, at].astype(F32)
            ).astype(BF16)
            return carry

        lax.fori_loop(0, per_half, step, 0)

    for which in range(2):
        sums[f"r{which}"]().wait_recv()
        sums[f"l{which}"]().wait_recv()
        finish(which)

    for k in range(4):
        own_right(k).wait_send()
        own_left(k).wait_send()
        forward(k).wait_send()
    for c in range(4):
        all_but_one(sent, c, send_sem)
        all_but_one(back_sent, c, back_send)
    for copy in sums.values():
        copy().wait_send()


def body(tokens, norm_gain, w_query, w_key, w_value, w_output, doc_lengths, pack_index):
    groups = lax.axis_size("dp")
    members = lax.axis_size("tp")
    rows, width = tokens.shape
    piece = width // 4
    q_cols, k_cols = w_query.shape[1], w_key.shape[1]
    total_cols = q_cols + 2 * k_cols
    per_kv = q_cols // k_cols
    side = (per_kv + 2) * HEAD_DIM
    ctx = per_kv * HEAD_DIM
    chunk_slots = SLOTS * groups
    index = jnp.swapaxes(pack_index.reshape(groups, members, rows), 0, 1)
    vmem = pl.BlockSpec(memory_space=pltpu.VMEM)
    hbm = pl.BlockSpec(memory_space=pl.ANY)
    dma = pltpu.SemaphoreType.DMA
    V = pltpu.VMEM
    return pl.pallas_call(
        kernel,
        out_shape=jax.ShapeDtypeStruct((rows, width), BF16),
        in_specs=[vmem, vmem, vmem, vmem, hbm, hbm, hbm, hbm],
        out_specs=vmem,
        scratch_shapes=[
            V((width, total_cols), BF16),
            V(w_output.shape, BF16),
            V((3, rows, width), BF16),
            V((rows, piece), BF16),
            V((4, rows, total_cols), F32),
            V((4, rows, 128), F32),
            V((2 * rows, side), BF16),
            V((4 * groups, 2 * SLOTS, side), BF16),
            V((4 * groups, 2 * SLOTS, side), BF16),
            V((2, 4 * chunk_slots, side), BF16),
            V((1, 4 * chunk_slots), F32),
            V((4, chunk_slots, 128), F32),
            V((4, chunk_slots, 128), F32),
            V((chunk_slots, 4 * chunk_slots), F32),
            V((4, 2 * rows, 2 * SLOTS * groups), BF16),
            V((2, chunk_slots, ctx), BF16),
            V((4 * groups, 2 * SLOTS, ctx), BF16),
            V((4 * groups, 2 * SLOTS, ctx), BF16),
            V((rows, 2 * ctx), BF16),
            V((3, rows, width), BF16),
            V((rows, width // 2), BF16),
            V((rows, width // 2), BF16),
            V((rows, width), BF16),
            V((rows, width), BF16),
            V((rows, width), F32),
            dma((3, 4)),
            dma,
            dma((3, 4)),
            dma((3, 4)),
            dma((4,)),
            dma((4,)),
            dma((4,)),
            dma((4,)),
            dma((6,)),
            dma((6,)),
        ],
        compiler_params=pltpu.CompilerParams(
            collective_id=0, has_side_effects=True, vmem_limit_bytes=67043328
        ),
        name="packed_attention",
    )(tokens, norm_gain.reshape(1, width), index, doc_lengths.reshape(1, -1), w_query, w_key, w_value, w_output)


def solution(mesh):
    placed = (
        P(("dp", "tp"), None),
        P(),
        P(None, "tp"),
        P(None, "tp"),
        P(None, "tp"),
        P("tp", None),
        P(),
        P(),
    )
    return jax.shard_map(
        body, mesh=mesh, in_specs=placed, out_specs=P(("dp", "tp"), None), check_vma=False
    )
```

```python
import functools
import math

import jax
import jax.numpy as jnp
from jax import lax
from jax.experimental import pallas as pl
from jax.experimental.pallas import tpu as pltpu
from jax.sharding import PartitionSpec as P

HEAD_DIM = 128
GROUP_DOCS = 4
SLOTS = 8
rope_base = 500000.0
norm_eps = 1e-05
score_floor = -1e30
MESH = pl.DeviceIdType.MESH
F32 = jnp.float32
BF16 = jnp.bfloat16


def iota(shape, dim):
    return lax.broadcasted_iota(jnp.int32, shape, dim)


def kernel(
    x_hbm, gain_hbm, pidx_hbm, len_hbm, wq_ref, wk_ref, wv_ref, wo_ref, out_hbm,
    x_ref, gain_ref, pidx_ref, len_ref, partner_x, out_ref,
    w_all, w_out, gathered, scaled, acc, sumsq, stacked, cosines, sines, picks, sent, arrived, qkv,
    slot_row, slot_col, slot_start, bias, unpack, mixed, back_sent, back, unpacked,
    part, half_a, half_b, from_left, from_right, own_part,
    in_sem, out_sem, w_sem, wo_sem, pair_send, pair_recv, ag_send, ag_recv,
    send_sem, recv_sem, back_send, back_recv, rs_send, rs_recv,
):
    groups = lax.axis_size("dp")
    rows, width = x_ref.shape
    piece = width // 4
    half = width // 2
    docs = len_ref.shape[1]
    me = lax.axis_index("dp")
    z = lax.axis_index("tp")
    right = lax.rem(z + 1, 4)
    left = lax.rem(z + 3, 4)
    core = lax.rem(me, 2)
    partner = me + 1 - 2 * core
    ahead = lax.rem(z + 1 + 2 * core, 4)
    behind = lax.rem(z + 3 - 2 * core, 4)
    first, second = core, 1 - core

    def member(c):
        return lax.rem(z + c // 3 * 2 + (c % 3 + 1) // 2 * (1 + 2 * (c % 2)), 4)

    q_cols = wq_ref.shape[1]
    k_cols = wk_ref.shape[1]
    heads = q_cols // HEAD_DIM
    kv_heads = k_cols // HEAD_DIM
    per_kv = heads // kv_heads
    side = (per_kv + 2) * HEAD_DIM
    ctx = per_kv * HEAD_DIM
    pack_rows = 2 * SLOTS
    nb = min(16, groups)
    chunk_slots = SLOTS * groups

    def cols(k):
        return pl.ds(k * piece, piece) if isinstance(k, int) else pl.ds(pl.multiple_of(k * piece, 128), piece)

    def w_copies(k):
        at = cols(k)
        return (
            pltpu.make_async_copy(wq_ref.at[at, :], w_all.at[at, pl.ds(0, q_cols)], w_sem.at[0, k]),
            pltpu.make_async_copy(wk_ref.at[at, :], w_all.at[at, pl.ds(q_cols, k_cols)], w_sem.at[1, k]),
            pltpu.make_async_copy(wv_ref.at[at, :], w_all.at[at, pl.ds(q_cols + k_cols, k_cols)], w_sem.at[2, k]),
        )

    loads = [
        pltpu.make_async_copy(src, dst, in_sem.at[i])
        for i, (src, dst) in enumerate(
            ((x_hbm, x_ref), (gain_hbm, gain_ref), (pidx_hbm, pidx_ref), (len_hbm, len_ref))
        )
    ]
    for copy in loads:
        copy.start()
    for k in range(4):
        for copy in w_copies(k):
            copy.start()
    wo_copy = pltpu.make_async_copy(wo_ref, w_out, wo_sem)
    wo_copy.start()

    barrier = pltpu.get_barrier_semaphore()

    def greet(i, carry):
        pl.semaphore_signal(barrier, inc=1, device_id=(lax.rem(me + i, groups), z), device_id_type=MESH)
        return carry

    for device in ((me, right), (me, left), (partner, ahead)):
        pl.semaphore_signal(barrier, inc=1, device_id=device, device_id_type=MESH)
    lax.fori_loop(1, groups, greet, 0)
    for copy in loads:
        copy.wait()
    pl.semaphore_wait(barrier, groups + 2)

    def copy_to(src, dst, send, recv, device):
        return pltpu.make_async_remote_copy(
            src_ref=src, dst_ref=dst, send_sem=send, recv_sem=recv, device_id=device, device_id_type=MESH
        )

    def column_copy(src, dst, send, recv, to):
        return copy_to(src, dst, send, recv, (me, to))

    def own_ahead(k):
        return copy_to(
            x_ref.at[:, cols(k)], gathered.at[first, :, cols(k)], ag_send.at[0, k], ag_recv.at[first, k], (me, ahead)
        )

    def to_partner(k):
        return copy_to(x_ref.at[:, cols(k)], partner_x.at[:, cols(k)], pair_send.at[k], pair_recv.at[k], (partner, z))

    def partner_ahead(k):
        return copy_to(
            partner_x.at[:, cols(k)], gathered.at[first, :, cols(k)], ag_send.at[1, k], ag_recv.at[first, k], (partner, ahead)
        )

    def landed(slot, k):
        piece_ref = gathered.at[slot, :, cols(k)]
        pltpu.make_async_copy(piece_ref, piece_ref, ag_recv.at[slot, k]).wait()

    def forward(slot, j, to):
        k = 2 * slot + j
        source = gathered.at[slot, :, cols(k)]
        return copy_to(source, gathered.at[2, :, cols(k)], ag_send.at[2, k], ag_recv.at[2, k], (me, to))

    for k in range(4):
        own_ahead(k).start()
        to_partner(k).start()

    lane = iota((1, docs), 1)
    lens_row = len_ref[...].astype(F32)
    eye_docs = iota((docs, docs), 0) == iota((docs, docs), 1)
    lens_col = jnp.sum(jnp.where(eye_docs, lens_row, 0.0), axis=1, keepdims=True)
    before = iota((docs, docs), 0) < iota((docs, docs), 1)
    starts_row = jnp.sum(jnp.where(before, lens_col, 0.0), axis=0, keepdims=True)
    group_of = iota((groups, docs), 0)
    lane_g = iota((groups, docs), 1)
    group_lo = jnp.sum(jnp.where(lane_g < GROUP_DOCS * group_of, lens_row, 0.0), axis=1, keepdims=True)
    group_hi = jnp.sum(jnp.where(lane_g < GROUP_DOCS * (group_of + 1), lens_row, 0.0), axis=1, keepdims=True)

    def upto(count):
        return jnp.sum(jnp.where(lane < count, lens_row, 0.0), axis=1, keepdims=True)

    my_lo = upto(GROUP_DOCS * me)
    my_hi = upto(GROUP_DOCS * (me + 1))
    my_starts = [upto(GROUP_DOCS * me + i) - my_lo for i in range(1, GROUP_DOCS)]
    earlier = (iota((rows, rows), 0) < iota((rows, rows), 1)).astype(BF16)
    spread_p = (iota((pack_rows * groups, groups), 0) // pack_rows == iota((pack_rows * groups, groups), 1)).astype(BF16)
    spread_s = (iota((chunk_slots, groups), 0) // SLOTS == iota((chunk_slots, groups), 1)).astype(BF16)

    def dot(a, b):
        return jnp.dot(a, b, preferred_element_type=F32)

    def slot_tables(c):
        index = pidx_ref[pl.ds(member(c), groups, stride=4), :].astype(F32)
        mine = (index >= my_lo) & (index < my_hi)
        rank = dot(jnp.where(mine, 1.0, 0.0).astype(BF16), earlier)
        code = jnp.where(mine, rank, -1.0).astype(BF16)
        place = jnp.where(mine, index - my_lo, 0.0)
        high = jnp.floor(place * (1.0 / 32.0))
        low = place - high * 32.0
        code_s = dot(spread_s, code)
        place_s = dot(spread_s, high.astype(BF16)) * 32.0 + dot(spread_s, low.astype(BF16))
        wanted = (iota((chunk_slots, rows), 0) % SLOTS).astype(F32)
        found = jnp.sum(jnp.where(code_s == wanted, place_s + 1.0, 0.0), axis=1, keepdims=True) - 1.0
        begin = jnp.zeros_like(found)
        for start in my_starts:
            begin = jnp.where(found >= start, start, begin)
        slot_col[c] = jnp.broadcast_to(found, (chunk_slots, 128))
        slot_start[c] = jnp.broadcast_to(begin, (chunk_slots, 128))
        same = iota((chunk_slots, chunk_slots), 0) == iota((chunk_slots, chunk_slots), 1)
        slot_row[:, pl.ds(c * chunk_slots, chunk_slots)] = jnp.sum(jnp.where(same, found, 0.0), axis=0, keepdims=True)

    sumsq[...] = jnp.zeros_like(sumsq)
    acc[...] = jnp.zeros_like(acc)
    total_cols = q_cols + 2 * k_cols
    n_tile = 512

    def project(c, k, x):
        at = cols(k)
        x = x.astype(F32)
        squares = sumsq[c]
        for j in range(piece // 128):
            block = x[:, j * 128 : (j + 1) * 128]
            squares = squares + block * block
        sumsq[c] = squares
        scaled[...] = (x * gain_ref[:, at]).astype(BF16)
        for n in range(total_cols // n_tile):
            to = pl.ds(n * n_tile, n_tile)
            acc[c, :, to] += dot(scaled[...], w_all[at, to])

    def prepare(c):
        index = pidx_ref[pl.ds(4 * me + member(c), 1), :].astype(F32)
        eye = iota((rows, rows), 0) == iota((rows, rows), 1)
        index_col = jnp.sum(jnp.where(eye, index, 0.0), axis=1, keepdims=True)
        begin = jnp.max(jnp.where(starts_row <= index_col, starts_row, 0.0), axis=1, keepdims=True)
        place = index_col - begin
        lanes = iota((1, HEAD_DIM), 1)
        exponent = (lanes % (HEAD_DIM // 2)).astype(F32) * (-2.0 * math.log(rope_base) / HEAD_DIM)
        angle = place * jnp.exp(exponent)
        cosines[c] = jnp.cos(angle)
        sines[c] = jnp.where(lanes < HEAD_DIM // 2, -1.0, 1.0) * jnp.sin(angle)
        inside = (index >= group_lo) & (index < group_hi)
        rank = dot(jnp.where(inside, 1.0, 0.0).astype(BF16), earlier)
        code = jnp.where(inside, rank, -100.0).astype(BF16)
        spread = dot(spread_p, code)
        wanted = (iota((pack_rows * groups, rows), 0) % pack_rows).astype(F32)
        for g in range(2):
            pick = jnp.where(spread + float(SLOTS * g) == wanted, 1.0, 0.0)
            unpack[c, pl.ds(g * rows, rows), :] = jnp.transpose(pick).astype(BF16)
            picks[c, :, pl.ds(g * rows, rows)] = pick.astype(BF16)

    def dispatch(c):
        scale = lax.rsqrt(jnp.sum(sumsq[c], axis=1, keepdims=True) * (1.0 / width) + norm_eps)
        cosine = cosines[c]
        sine = sines[c]
        query_scale = scale * (HEAD_DIM ** (-0.5) / math.log(2.0))

        def head(column, by):
            return acc[c, :, pl.ds(column * HEAD_DIM, HEAD_DIM)] * by

        def rope(t):
            return t * cosine + pltpu.roll(t, HEAD_DIM // 2, 1) * sine

        for g in range(kv_heads):
            at = pl.ds(g * rows, rows)
            for j in range(per_kv):
                stacked[at, pl.ds(j * HEAD_DIM, HEAD_DIM)] = rope(head(g * per_kv + j, query_scale)).astype(BF16)
            stacked[at, pl.ds(ctx, HEAD_DIM)] = rope(head(heads + g, scale)).astype(BF16)
            stacked[at, pl.ds(ctx + HEAD_DIM, HEAD_DIM)] = head(heads + kv_heads + g, scale).astype(BF16)
        for b in range(groups // nb):
            block = picks[c, pl.ds(b * nb * pack_rows, nb * pack_rows), :]
            sent[pl.ds(c * groups + b * nb, nb)] = (
                dot(block, stacked[...]).astype(BF16).reshape(nb, pack_rows, side)
            )
        arrived[c * groups + me] = sent[c * groups + me]

        def send(i, carry):
            to = lax.rem(me + i, groups)
            pltpu.make_async_remote_copy(
                src_ref=sent.at[c * groups + to],
                dst_ref=arrived.at[c * groups + me],
                send_sem=send_sem.at[c],
                recv_sem=recv_sem.at[c],
                device_id=(to, z),
                device_id_type=MESH,
            ).start()
            return carry

        lax.fori_loop(1, groups, send, 0)

    def all_but_one(ref, c, sem):
        block = ref.at[pl.ds(c * groups, groups - 1)]
        pltpu.make_async_copy(block, block, sem.at[c]).wait()

    reorder_rows = pack_rows * nb
    out_row = iota((reorder_rows, reorder_rows), 0)
    in_row = iota((reorder_rows, reorder_rows), 1)
    split = nb * SLOTS
    source_row = (out_row % split) // SLOTS * pack_rows + out_row // split * SLOTS + out_row % SLOTS
    apart = (source_row == in_row).astype(BF16)
    source_back = (in_row % split) // SLOTS * pack_rows + in_row // split * SLOTS + in_row % SLOTS
    together = (source_back == out_row).astype(BF16)

    def receive(c):
        all_but_one(arrived, c, recv_sem)
        for b in range(groups // nb):
            block = arrived[pl.ds(c * groups + b * nb, nb)].reshape(reorder_rows, side)
            ordered = dot(apart, block).astype(BF16)
            for g in range(2):
                qkv[g, pl.ds(c * chunk_slots + b * split, split), pl.ds(0, side)] = ordered[g * split : (g + 1) * split]

    def mask(c):
        found = slot_col[c][:, :1]
        begin = slot_start[c][:, :1]
        keys = slot_row[...]
        bias[...] = jnp.where((keys >= begin) & (keys <= found), 0.0, score_floor)

    def attend(c):
        at = pl.ds(c * chunk_slots, chunk_slots)

        for i in range(heads):
            g = i // per_kv
            lanes = pl.ds(i % per_kv * HEAD_DIM, HEAD_DIM)
            query = qkv[g, at, lanes]
            key = qkv[g, :, pl.ds(ctx, HEAD_DIM)]
            value = qkv[g, :, pl.ds(ctx + HEAD_DIM, 2 * HEAD_DIM)]
            scores = lax.dot_general(query, key, (((1,), (1,)), ((), ())), preferred_element_type=F32)
            scores = scores + bias[...]
            weights = jnp.exp2(scores - jnp.max(scores, axis=1, keepdims=True))
            both = dot(weights.astype(BF16), value)
            mixed[g, :, lanes] = (both[:, :HEAD_DIM] / both[:, HEAD_DIM:]).astype(BF16)
        for b in range(groups // nb):
            block = mixed[:, pl.ds(b * split, split), :].reshape(reorder_rows, ctx)
            back_sent[pl.ds(c * groups + b * nb, nb)] = dot(together, block).astype(BF16).reshape(nb, pack_rows, ctx)
        back[c * groups + me] = back_sent[c * groups + me]

        def send(i, carry):
            to = lax.rem(me + i, groups)
            pltpu.make_async_remote_copy(
                src_ref=back_sent.at[c * groups + to],
                dst_ref=back.at[c * groups + me],
                send_sem=back_send.at[c],
                recv_sem=back_recv.at[c],
                device_id=(to, z),
                device_id_type=MESH,
            ).start()
            return carry

        lax.fori_loop(1, groups, send, 0)

    o_tile = min(512, half)
    per_half = half // o_tile

    def fetch(c):
        all_but_one(back, c, back_recv)
        block = back[pl.ds(c * groups, groups)].reshape(pack_rows * groups, ctx)
        both = dot(unpack[c], block).astype(BF16)
        for g in range(2):
            unpacked[c, :, pl.ds(g * ctx, ctx)] = both[g * rows : (g + 1) * rows]

    def tile(n):
        return pl.ds(pl.multiple_of(n * o_tile, 128), o_tile)

    def output_half(c, which, extra):
        def step(n, carry):
            at = tile(which * per_half + n)
            value = dot(unpacked[c], w_out[:, at])
            if extra is not None:
                value = value + extra[:, tile(n)].astype(F32)
            part[c - 1, :, at] = value.astype(BF16)
            return carry

        lax.fori_loop(0, per_half, step, 0)

    halves = (pl.ds(0, half), pl.ds(half, half))
    sums = {
        "a": lambda: column_copy(part.at[2, :, halves[0]], half_a, rs_send.at[0], rs_recv.at[0], right),
        "b": lambda: column_copy(part.at[2, :, halves[1]], half_b, rs_send.at[1], rs_recv.at[1], left),
        "r0": lambda: column_copy(part.at[1, :, halves[0]], from_left.at[:, halves[0]], rs_send.at[2], rs_recv.at[2], right),
        "r1": lambda: column_copy(part.at[1, :, halves[1]], from_left.at[:, halves[1]], rs_send.at[3], rs_recv.at[3], right),
        "l0": lambda: column_copy(part.at[0, :, halves[0]], from_right.at[:, halves[0]], rs_send.at[4], rs_recv.at[4], left),
        "l1": lambda: column_copy(part.at[0, :, halves[1]], from_right.at[:, halves[1]], rs_send.at[5], rs_recv.at[5], left),
    }

    for k in range(4):
        for copy in w_copies(k):
            copy.wait()
        project(0, k, x_ref[:, cols(k)])
    prepare(0)
    dispatch(0)
    for k in range(4):
        to_partner(k).wait_recv()
        partner_ahead(k).start()
    for c in range(1, 4):
        prepare(c)
    for c in range(4):
        slot_tables(c)
    for g in range(2):
        qkv[g, :, pl.ds(side, HEAD_DIM)] = jnp.ones((4 * chunk_slots, HEAD_DIM), BF16)
    mask(3)

    def first_piece(k, carry):
        landed(first, k)
        project(1 + first, k, gathered[first, :, cols(k)])
        return carry

    lax.fori_loop(0, 4, first_piece, 0)
    for j in range(2):
        forward(first, j, ahead).start()
    dispatch(1 + first)
    receive(0)

    def second_piece(k, carry):
        landed(second, k)
        project(1 + second, k, gathered[second, :, cols(k)])
        return carry

    lax.fori_loop(0, 4, second_piece, 0)
    for j in range(2):
        forward(second, j, behind).start()
    dispatch(1 + second)

    def far_piece(i, carry):
        k = i % 2 * 2 + i // 2
        landed(2, k)
        project(3, k, gathered[2, :, cols(k)])
        return carry

    lax.fori_loop(0, 4, far_piece, 0)
    dispatch(3)
    receive(1)
    receive(2)
    receive(3)
    wo_copy.wait()
    attend(3)
    mask(2)
    attend(2)
    mask(1)
    attend(1)
    mask(0)
    fetch(3)
    output_half(3, 0, None)
    sums["a"]().start()
    output_half(3, 1, None)
    sums["b"]().start()
    attend(0)
    fetch(2)
    output_half(2, 1, None)
    sums["r1"]().start()
    fetch(1)
    output_half(1, 0, None)
    sums["l0"]().start()
    sums["a"]().wait_recv()
    output_half(2, 0, half_a)
    sums["r0"]().start()
    sums["b"]().wait_recv()
    output_half(1, 1, half_b)
    sums["l1"]().start()
    fetch(0)

    def own_step(n, carry):
        at = tile(n)
        own_part[:, at] = x_ref[:, at].astype(F32) + dot(unpacked[0], w_out[:, at])
        return carry

    lax.fori_loop(0, 2 * per_half, own_step, 0)

    def finish(which):
        def step(n, carry):
            at = tile(which * per_half + n)
            out_ref[:, at] = (
                own_part[:, at] + from_left[:, at].astype(F32) + from_right[:, at].astype(F32)
            ).astype(BF16)
            return carry

        lax.fori_loop(0, per_half, step, 0)

    stores = [
        pltpu.make_async_copy(out_ref.at[:, halves[i]], out_hbm.at[:, halves[i]], out_sem.at[i]) for i in range(2)
    ]
    for which in range(2):
        sums[f"r{which}"]().wait_recv()
        sums[f"l{which}"]().wait_recv()
        finish(which)
        stores[which].start()

    for k in range(4):
        own_ahead(k).wait_send()
        to_partner(k).wait_send()
        partner_ahead(k).wait_send()
    for j in range(2):
        forward(first, j, ahead).wait_send()
        forward(second, j, behind).wait_send()
    for c in range(4):
        all_but_one(sent, c, send_sem)
        all_but_one(back_sent, c, back_send)
    for copy in sums.values():
        copy().wait_send()
    for copy in stores:
        copy.wait()


def body(tokens, norm_gain, w_query, w_key, w_value, w_output, doc_lengths, pack_index):
    groups = lax.axis_size("dp")
    members = lax.axis_size("tp")
    rows, width = tokens.shape
    piece = width // 4
    q_cols, k_cols = w_query.shape[1], w_key.shape[1]
    total_cols = q_cols + 2 * k_cols
    per_kv = q_cols // k_cols
    side = (per_kv + 2) * HEAD_DIM
    ctx = per_kv * HEAD_DIM
    chunk_slots = SLOTS * groups
    index = pack_index.reshape(groups * members, rows)
    hbm = pl.BlockSpec(memory_space=pl.ANY)
    dma = pltpu.SemaphoreType.DMA
    V = pltpu.VMEM
    return pl.pallas_call(
        kernel,
        out_shape=jax.ShapeDtypeStruct((rows, width), BF16),
        in_specs=[hbm] * 8,
        out_specs=hbm,
        scratch_shapes=[
            V((rows, width), BF16),
            V((1, width), F32),
            V((groups * members, rows), jnp.int32),
            V((1, doc_lengths.shape[0]), jnp.int32),
            V((rows, width), BF16),
            V((rows, width), BF16),
            V((width, total_cols), BF16),
            V(w_output.shape, BF16),
            V((3, rows, width), BF16),
            V((rows, piece), BF16),
            V((4, rows, total_cols), F32),
            V((4, rows, 128), F32),
            V((2 * rows, side), BF16),
            V((4, rows, HEAD_DIM), F32),
            V((4, rows, HEAD_DIM), F32),
            V((4, 2 * SLOTS * groups, 2 * rows), BF16),
            V((4 * groups, 2 * SLOTS, side), BF16),
            V((4 * groups, 2 * SLOTS, side), BF16),
            V((2, 4 * chunk_slots, side + HEAD_DIM), BF16),
            V((1, 4 * chunk_slots), F32),
            V((4, chunk_slots, 128), F32),
            V((4, chunk_slots, 128), F32),
            V((chunk_slots, 4 * chunk_slots), F32),
            V((4, 2 * rows, 2 * SLOTS * groups), BF16),
            V((2, chunk_slots, ctx), BF16),
            V((4 * groups, 2 * SLOTS, ctx), BF16),
            V((4 * groups, 2 * SLOTS, ctx), BF16),
            V((4, rows, 2 * ctx), BF16),
            V((3, rows, width), BF16),
            V((rows, width // 2), BF16),
            V((rows, width // 2), BF16),
            V((rows, width), BF16),
            V((rows, width), BF16),
            V((rows, width), F32),
            dma((4,)),
            dma((2,)),
            dma((3, 4)),
            dma,
            dma((4,)),
            dma((4,)),
            dma((3, 4)),
            dma((3, 4)),
            dma((4,)),
            dma((4,)),
            dma((4,)),
            dma((4,)),
            dma((6,)),
            dma((6,)),
        ],
        compiler_params=pltpu.CompilerParams(
            collective_id=0, has_side_effects=True, vmem_limit_bytes=67043328
        ),
        name="packed_attention",
    )(tokens, norm_gain.reshape(1, width), index, doc_lengths.reshape(1, -1), w_query, w_key, w_value, w_output)


def solution(mesh):
    placed = (
        P(("dp", "tp"), None),
        P(),
        P(None, "tp"),
        P(None, "tp"),
        P(None, "tp"),
        P("tp", None),
        P(),
        P(),
    )
    return jax.shard_map(
        body, mesh=mesh, in_specs=placed, out_specs=P(("dp", "tp"), None), check_vma=False
    )
```

```python
import functools
import math

import jax
import jax.numpy as jnp
from jax import lax
from jax.experimental import pallas as pl
from jax.experimental.pallas import tpu as pltpu
from jax.sharding import PartitionSpec as P

HEAD_DIM = 128
GROUP_DOCS = 4
SLOTS = 8
rope_base = 500000.0
norm_eps = 1e-05
score_floor = -1e30
MESH = pl.DeviceIdType.MESH
F32 = jnp.float32
BF16 = jnp.bfloat16


def iota(shape, dim):
    return lax.broadcasted_iota(jnp.int32, shape, dim)


def kernel(
    x_hbm, gain_hbm, pidx_hbm, len_hbm, wq_ref, wk_ref, wv_ref, wo_ref,
    out_hbm,
    x_ref, gain_ref, pidx_ref, len_ref, partner_x,
    w_all, w_out, gathered, scaled, acc, sumsq, stacked, cosines, sines, picks, sent, arrived, qkv,
    slot_row, slot_col, slot_start, bias, unpack, mixed, back_sent, back, unpacked,
    part, half_a, half_b, from_behind, from_ahead, own_part, early, early_peak,
    in_sem, out_sem, w_sem, wo_sem, pair_send, pair_recv, ag_send, ag_recv,
    send_sem, recv_sem, back_send, back_recv, rs_send, rs_recv,
):
    groups = lax.axis_size("dp")
    rows, width = x_ref.shape
    piece = width // 4
    half = width // 2
    docs = len_ref.shape[1]
    me = lax.axis_index("dp")
    z = lax.axis_index("tp")
    right = lax.rem(z + 1, 4)
    left = lax.rem(z + 3, 4)
    core = lax.rem(me, 2)
    partner = me + 1 - 2 * core
    ahead = lax.rem(z + 1 + 2 * core, 4)
    behind = lax.rem(z + 3 - 2 * core, 4)
    own, first, second, far = 0, 1, 2, 3

    def member(c, parity):
        return lax.rem(z + (0, 3 - 2 * parity, 1 + 2 * parity, 2)[c], 4)

    q_cols = wq_ref.shape[1]
    k_cols = wk_ref.shape[1]
    heads = q_cols // HEAD_DIM
    kv_heads = k_cols // HEAD_DIM
    per_kv = heads // kv_heads
    side = (per_kv + 2) * HEAD_DIM
    ctx = per_kv * HEAD_DIM
    pack_rows = 2 * SLOTS
    nb = min(16, groups)
    chunk_slots = SLOTS * groups

    def cols(k):
        return pl.ds(k * piece, piece) if isinstance(k, int) else pl.ds(pl.multiple_of(k * piece, 128), piece)

    def w_copies(k):
        at = cols(k)
        return (
            pltpu.make_async_copy(wq_ref.at[at, :], w_all.at[at, pl.ds(0, q_cols)], w_sem.at[0, k]),
            pltpu.make_async_copy(wk_ref.at[at, :], w_all.at[at, pl.ds(q_cols, k_cols)], w_sem.at[1, k]),
            pltpu.make_async_copy(wv_ref.at[at, :], w_all.at[at, pl.ds(q_cols + k_cols, k_cols)], w_sem.at[2, k]),
        )

    loads = [
        pltpu.make_async_copy(src, dst, in_sem.at[i])
        for i, (src, dst) in enumerate(
            ((x_hbm, x_ref), (gain_hbm, gain_ref), (pidx_hbm, pidx_ref), (len_hbm, len_ref))
        )
    ]
    for copy in loads:
        copy.start()
    for k in range(4):
        for copy in w_copies(k):
            copy.start()
    wo_copy = pltpu.make_async_copy(wo_ref, w_out, wo_sem)
    wo_copy.start()

    barrier = pltpu.get_barrier_semaphore()

    def greet(i, carry):
        pl.semaphore_signal(barrier, inc=1, device_id=(lax.rem(me + i, groups), z), device_id_type=MESH)
        return carry

    for device in ((me, right), (me, left), (partner, ahead)):
        pl.semaphore_signal(barrier, inc=1, device_id=device, device_id_type=MESH)
    lax.fori_loop(1, groups, greet, 0)
    for copy in loads:
        copy.wait()
    pl.semaphore_wait(barrier, groups + 2)

    def copy_to(src, dst, send, recv, device):
        return pltpu.make_async_remote_copy(
            src_ref=src, dst_ref=dst, send_sem=send, recv_sem=recv, device_id=device, device_id_type=MESH
        )

    def column_copy(src, dst, send, recv, to):
        return copy_to(src, dst, send, recv, (me, to))

    def own_ahead(k):
        return copy_to(
            x_ref.at[:, cols(k)], gathered.at[0, :, cols(k)], ag_send.at[0, k], ag_recv.at[0, k], (me, ahead)
        )

    def to_partner(k):
        return copy_to(x_ref.at[:, cols(k)], partner_x.at[:, cols(k)], pair_send.at[k], pair_recv.at[k], (partner, z))

    def partner_ahead(k):
        return copy_to(
            partner_x.at[:, cols(k)], gathered.at[1, :, cols(k)], ag_send.at[1, k], ag_recv.at[1, k], (partner, ahead)
        )

    def landed(c, k):
        piece_ref = gathered.at[c - 1, :, cols(k)]
        pltpu.make_async_copy(piece_ref, piece_ref, ag_recv.at[c - 1, k]).wait()

    def forward(k):
        source = gathered.at[k // 2, :, cols(k)]
        to = (ahead, behind)[k // 2]
        return copy_to(source, gathered.at[2, :, cols(k)], ag_send.at[2, k], ag_recv.at[2, k], (me, to))

    for k in range(4):
        own_ahead(k).start()
        to_partner(k).start()

    lane = iota((1, docs), 1)
    lens_row = len_ref[...].astype(F32)
    eye_docs = iota((docs, docs), 0) == iota((docs, docs), 1)
    lens_col = jnp.sum(jnp.where(eye_docs, lens_row, 0.0), axis=1, keepdims=True)
    before = iota((docs, docs), 0) < iota((docs, docs), 1)
    starts_row = jnp.sum(jnp.where(before, lens_col, 0.0), axis=0, keepdims=True)
    group_of = iota((groups, docs), 0)
    lane_g = iota((groups, docs), 1)
    group_lo = jnp.sum(jnp.where(lane_g < GROUP_DOCS * group_of, lens_row, 0.0), axis=1, keepdims=True)
    group_hi = jnp.sum(jnp.where(lane_g < GROUP_DOCS * (group_of + 1), lens_row, 0.0), axis=1, keepdims=True)

    def upto(count):
        return jnp.sum(jnp.where(lane < count, lens_row, 0.0), axis=1, keepdims=True)

    my_lo = upto(GROUP_DOCS * me)
    my_hi = upto(GROUP_DOCS * (me + 1))
    my_starts = [upto(GROUP_DOCS * me + i) - my_lo for i in range(1, GROUP_DOCS)]
    earlier = (iota((rows, rows), 0) < iota((rows, rows), 1)).astype(BF16)
    spread_p = (iota((pack_rows * groups, groups), 0) // pack_rows == iota((pack_rows * groups, groups), 1)).astype(BF16)
    spread_s = (iota((chunk_slots, groups), 0) // SLOTS == iota((chunk_slots, groups), 1)).astype(BF16)

    def dot(a, b):
        return jnp.dot(a, b, preferred_element_type=F32)

    def slot_tables(c):
        index = pidx_ref[pl.ds(member(c, 0), groups, stride=4), :]
        if c in (first, second):
            odd = iota((groups, rows), 0) % 2 == 1
            index = jnp.where(odd, pidx_ref[pl.ds(member(c, 1), groups, stride=4), :], index)
        index = index.astype(F32)
        mine = (index >= my_lo) & (index < my_hi)
        rank = dot(jnp.where(mine, 1.0, 0.0).astype(BF16), earlier)
        code = jnp.where(mine, rank, -1.0).astype(BF16)
        place = jnp.where(mine, index - my_lo, 0.0)
        high = jnp.floor(place * (1.0 / 32.0))
        low = place - high * 32.0
        code_s = dot(spread_s, code)
        place_s = dot(spread_s, high.astype(BF16)) * 32.0 + dot(spread_s, low.astype(BF16))
        wanted = (iota((chunk_slots, rows), 0) % SLOTS).astype(F32)
        found = jnp.sum(jnp.where(code_s == wanted, place_s + 1.0, 0.0), axis=1, keepdims=True) - 1.0
        begin = jnp.zeros_like(found)
        for start in my_starts:
            begin = jnp.where(found >= start, start, begin)
        slot_col[c] = jnp.broadcast_to(found, (chunk_slots, 128))
        slot_start[c] = jnp.broadcast_to(begin, (chunk_slots, 128))
        same = iota((chunk_slots, chunk_slots), 0) == iota((chunk_slots, chunk_slots), 1)
        slot_row[:, pl.ds(c * chunk_slots, chunk_slots)] = jnp.sum(jnp.where(same, found, 0.0), axis=0, keepdims=True)

    sumsq[...] = jnp.zeros_like(sumsq)
    acc[...] = jnp.zeros_like(acc)
    total_cols = q_cols + 2 * k_cols
    n_tile = 512

    n_tiles = total_cols // n_tile

    def scale_piece(c, k, slot, x):
        x = x.astype(F32)
        squares = sumsq[c]
        for j in range(piece // 128):
            block = x[:, j * 128 : (j + 1) * 128]
            squares = squares + block * block
        sumsq[c] = squares
        scaled[slot] = (x * gain_ref[:, cols(k)]).astype(BF16)

    def multiply(c, k, slot, tiles):
        for n in tiles:
            to = pl.ds(n * n_tile, n_tile)
            acc[c, :, to] += dot(scaled[slot], w_all[cols(k), to])

    def project(c, k, x):
        scale_piece(c, k, 0, x)
        multiply(c, k, 0, range(n_tiles))

    def prepare(c):
        index = pidx_ref[pl.ds(4 * me + member(c, core), 1), :].astype(F32)
        eye = iota((rows, rows), 0) == iota((rows, rows), 1)
        index_col = jnp.sum(jnp.where(eye, index, 0.0), axis=1, keepdims=True)
        begin = jnp.max(jnp.where(starts_row <= index_col, starts_row, 0.0), axis=1, keepdims=True)
        place = index_col - begin
        lanes = iota((1, HEAD_DIM), 1)
        exponent = (lanes % (HEAD_DIM // 2)).astype(F32) * (-2.0 * math.log(rope_base) / HEAD_DIM)
        angle = place * jnp.exp(exponent)
        cosines[c] = jnp.cos(angle)
        sines[c] = jnp.where(lanes < HEAD_DIM // 2, -1.0, 1.0) * jnp.sin(angle)
        inside = (index >= group_lo) & (index < group_hi)
        rank = dot(jnp.where(inside, 1.0, 0.0).astype(BF16), earlier)
        code = jnp.where(inside, rank, -100.0).astype(BF16)
        spread = dot(spread_p, code)
        wanted = (iota((pack_rows * groups, rows), 0) % pack_rows).astype(F32)
        for g in range(2):
            pick = jnp.where(spread + float(SLOTS * g) == wanted, 1.0, 0.0)
            unpack[c, pl.ds(g * rows, rows), :] = jnp.transpose(pick).astype(BF16)
            picks[c, :, pl.ds(g * rows, rows)] = pick.astype(BF16)

    query_lanes = pl.ds(0, ctx)
    pair_lanes = pl.ds(ctx, 2 * HEAD_DIM)
    all_lanes = pl.ds(0, side)

    def rotate_pairs(c, kind):
        scale = lax.rsqrt(jnp.sum(sumsq[c], axis=1, keepdims=True) * (1.0 / width) + norm_eps)
        cosine = cosines[c]
        sine = sines[c]
        query_scale = scale * (HEAD_DIM ** (-0.5) / math.log(2.0))

        def head(column, by):
            return acc[c, :, pl.ds(column * HEAD_DIM, HEAD_DIM)] * by

        def rope(t):
            return t * cosine + pltpu.roll(t, HEAD_DIM // 2, 1) * sine

        for g in range(kv_heads):
            at = pl.ds(g * rows, rows)
            if kind != "pair":
                for j in range(per_kv):
                    stacked[at, pl.ds(j * HEAD_DIM, HEAD_DIM)] = rope(head(g * per_kv + j, query_scale)).astype(BF16)
            if kind != "query":
                stacked[at, pl.ds(ctx, HEAD_DIM)] = rope(head(heads + g, scale)).astype(BF16)
                stacked[at, pl.ds(ctx + HEAD_DIM, HEAD_DIM)] = head(heads + kv_heads + g, scale).astype(BF16)

    def dispatch(c, kind="all"):
        lanes, sem = {"all": (all_lanes, c), "pair": (pair_lanes, c), "query": (query_lanes, 4)}[kind]
        rotate_pairs(c, kind)
        for b in range(groups // nb):
            block = picks[c, pl.ds(b * nb * pack_rows, nb * pack_rows), :]
            packed = dot(block, stacked[:, lanes]).astype(BF16)
            sent[pl.ds(c * groups + b * nb, nb), :, lanes] = packed.reshape(nb, pack_rows, packed.shape[1])
        arrived[c * groups + me, :, lanes] = sent[c * groups + me, :, lanes]

        def send(i, carry):
            to = lax.rem(me + i, groups)
            pltpu.make_async_remote_copy(
                src_ref=sent.at[c * groups + to, :, lanes],
                dst_ref=arrived.at[c * groups + me, :, lanes],
                send_sem=send_sem.at[sem],
                recv_sem=recv_sem.at[sem],
                device_id=(to, z),
                device_id_type=MESH,
            ).start()
            return carry

        lax.fori_loop(1, groups, send, 0)

    def all_but_one(ref, c, lanes, sem):
        block = ref.at[pl.ds(c * groups, groups - 1), :, lanes]
        pltpu.make_async_copy(block, block, sem).wait()

    reorder_rows = pack_rows * nb
    out_row = iota((reorder_rows, reorder_rows), 0)
    in_row = iota((reorder_rows, reorder_rows), 1)
    split = nb * SLOTS
    source_row = (out_row % split) // SLOTS * pack_rows + out_row // split * SLOTS + out_row % SLOTS
    apart = (source_row == in_row).astype(BF16)
    source_back = (in_row % split) // SLOTS * pack_rows + in_row // split * SLOTS + in_row % SLOTS
    together = (source_back == out_row).astype(BF16)

    def receive(c, kind="all"):
        lanes, sem = {"all": (all_lanes, c), "pair": (pair_lanes, c), "query": (query_lanes, 4)}[kind]
        all_but_one(arrived, c, lanes, recv_sem.at[sem])
        for b in range(groups // nb):
            block = arrived[pl.ds(c * groups + b * nb, nb), :, lanes]
            ordered = dot(apart, block.reshape(reorder_rows, block.shape[2])).astype(BF16)
            for g in range(2):
                qkv[g, pl.ds(c * chunk_slots + b * split, split), lanes] = ordered[g * split : (g + 1) * split]

    def mask(c):
        found = slot_col[c][:, :1]
        begin = slot_start[c][:, :1]
        keys = slot_row[...]
        bias[...] = jnp.where((keys >= begin) & (keys <= found), 0.0, score_floor)

    early_keys = pl.ds(0, far * chunk_slots)
    late_keys = pl.ds(far * chunk_slots, chunk_slots)
    every_key = pl.ds(0, 4 * chunk_slots)

    def scored(c, i, keys):
        g = i // per_kv
        query = qkv[g, pl.ds(c * chunk_slots, chunk_slots), pl.ds(i % per_kv * HEAD_DIM, HEAD_DIM)]
        key = qkv[g, keys, pl.ds(ctx, HEAD_DIM)]
        scores = lax.dot_general(query, key, (((1,), (1,)), ((), ())), preferred_element_type=F32)
        scores = scores + bias[:, keys]
        return scores, jnp.max(scores, axis=1, keepdims=True)

    def weighted(i, scores, peak, keys):
        weights = jnp.exp2(scores - peak).astype(BF16)
        return dot(weights, qkv[i // per_kv, keys, pl.ds(ctx + HEAD_DIM, 2 * HEAD_DIM)])

    def attend_early(c):
        for i in range(heads):
            scores, peak = scored(c, i, early_keys)
            early[i] = weighted(i, scores, peak, early_keys)
            early_peak[i] = jnp.broadcast_to(peak, (chunk_slots, HEAD_DIM))

    def attend(c, resumed=False):
        for i in range(heads):
            keys = late_keys if resumed else every_key
            scores, peak = scored(c, i, keys)
            if resumed:
                before = early_peak[i][:, :1]
                peak = jnp.maximum(peak, before)
                both = early[i] * jnp.exp2(before - peak) + weighted(i, scores, peak, keys)
            else:
                both = weighted(i, scores, peak, keys)
            mixed[i // per_kv, :, pl.ds(i % per_kv * HEAD_DIM, HEAD_DIM)] = (
                both[:, :HEAD_DIM] / both[:, HEAD_DIM:]
            ).astype(BF16)
        for b in range(groups // nb):
            block = mixed[:, pl.ds(b * split, split), :].reshape(reorder_rows, ctx)
            back_sent[pl.ds(c * groups + b * nb, nb)] = dot(together, block).astype(BF16).reshape(nb, pack_rows, ctx)
        back[c * groups + me] = back_sent[c * groups + me]

        def send(i, carry):
            to = lax.rem(me + i, groups)
            pltpu.make_async_remote_copy(
                src_ref=back_sent.at[c * groups + to],
                dst_ref=back.at[c * groups + me],
                send_sem=back_send.at[c],
                recv_sem=back_recv.at[c],
                device_id=(to, z),
                device_id_type=MESH,
            ).start()
            return carry

        lax.fori_loop(1, groups, send, 0)

    o_tile = min(512, half // 2)
    per_half = half // o_tile

    def fetch(c):
        all_but_one(back, c, query_lanes, back_recv.at[c])
        block = back[pl.ds(c * groups, groups)].reshape(pack_rows * groups, ctx)
        both = dot(unpack[c], block).astype(BF16)
        for g in range(2):
            unpacked[c, :, pl.ds(g * ctx, ctx)] = both[g * rows : (g + 1) * rows]

    def tile(n):
        return pl.ds(pl.multiple_of(n * o_tile, 128), o_tile)

    def output_part(c, which, extra, share=0, of=1):
        def step(n, carry):
            at = tile(which * per_half + n)
            value = dot(unpacked[c], w_out[:, at])
            if extra is not None:
                value = value + extra[:, tile(n)].astype(F32)
            part[c - 1, :, at] = value.astype(BF16)
            return carry

        lax.fori_loop(share * per_half // of, (share + 1) * per_half // of, step, 0)

    halves = (pl.ds(0, half), pl.ds(half, half))
    low, high = halves
    one, two, third, fourth = (pl.ds(i * (half // 2), half // 2) for i in range(4))
    sums = {
        "far_low": lambda: column_copy(part.at[2, :, low], half_a, rs_send.at[0], rs_recv.at[0], ahead),
        "far_high": lambda: column_copy(part.at[2, :, high], half_b, rs_send.at[1], rs_recv.at[1], behind),
        "second_one": lambda: column_copy(part.at[1, :, one], from_behind.at[:, one], rs_send.at[2], rs_recv.at[2], ahead),
        "second_two": lambda: column_copy(part.at[1, :, two], from_behind.at[:, two], rs_send.at[7], rs_recv.at[7], ahead),
        "second_third": lambda: column_copy(part.at[1, :, third], from_behind.at[:, third], rs_send.at[3], rs_recv.at[3], ahead),
        "second_fourth": lambda: column_copy(part.at[1, :, fourth], from_behind.at[:, fourth], rs_send.at[6], rs_recv.at[6], ahead),
        "first_low": lambda: column_copy(part.at[0, :, low], from_ahead.at[:, low], rs_send.at[4], rs_recv.at[4], behind),
        "first_third": lambda: column_copy(part.at[0, :, third], from_ahead.at[:, third], rs_send.at[5], rs_recv.at[5], behind),
        "first_fourth": lambda: column_copy(part.at[0, :, fourth], from_ahead.at[:, fourth], rs_send.at[8], rs_recv.at[8], behind),
    }

    for k in range(4):
        for copy in w_copies(k):
            copy.wait()
        project(0, k, x_ref[:, cols(k)])
    prepare(0)
    dispatch(0)
    for k in range(4):
        to_partner(k).wait_recv()
        partner_ahead(k).start()
    for c in range(1, 4):
        prepare(c)
    for c in range(4):
        slot_tables(c)
    for g in range(2):
        qkv[g, :, pl.ds(side, HEAD_DIM)] = jnp.ones((4 * chunk_slots, HEAD_DIM), BF16)
    mask(second)

    def first_piece(k, carry):
        landed(first, k)
        project(first, k, gathered[0, :, cols(k)])
        return carry

    lax.fori_loop(0, 4, first_piece, 0)
    for k in range(2):
        forward(k).start()
    dispatch(first)
    receive(own)

    def second_piece(k, carry):
        landed(second, k)
        project(second, k, gathered[1, :, cols(k)])
        return carry

    lax.fori_loop(0, 4, second_piece, 0)
    for k in range(2, 4):
        forward(k).start()
    dispatch(second)

    def far_piece(i, carry):
        landed(far, 2 * i)
        project(far, 2 * i, gathered[2, :, cols(2 * i)])
        return carry

    lax.fori_loop(0, 2, far_piece, 0)
    for i in range(2):
        k = 2 * i + 1
        landed(far, k)
        scale_piece(far, k, i, gathered[2, :, cols(k)])
        multiply(far, k, i, range(n_tiles - 1, n_tiles))
    dispatch(far, "pair")
    for i in range(2):
        multiply(far, 2 * i + 1, i, range(n_tiles - 1))
    dispatch(far, "query")
    receive(first)
    receive(second)
    attend_early(second)
    receive(far, "pair")
    attend(second, True)
    mask(far)
    receive(far, "query")
    attend(far)
    mask(first)
    wo_copy.wait()
    fetch(second)
    output_part(second, 1, None, 0, 2)
    sums["second_third"]().start()
    output_part(second, 1, None, 1, 2)
    sums["second_fourth"]().start()
    attend(first)
    mask(own)
    fetch(far)
    output_part(far, 0, None)
    sums["far_low"]().start()
    output_part(far, 1, None)
    sums["far_high"]().start()
    attend(own)
    fetch(first)
    output_part(first, 0, None)
    sums["first_low"]().start()
    sums["far_low"]().wait_recv()
    output_part(second, 0, half_a, 0, 2)
    sums["second_one"]().start()
    output_part(second, 0, half_a, 1, 2)
    sums["second_two"]().start()
    sums["far_high"]().wait_recv()
    output_part(first, 1, half_b, 0, 2)
    sums["first_third"]().start()
    output_part(first, 1, half_b, 1, 2)
    sums["first_fourth"]().start()
    fetch(own)

    def own_step(n, carry):
        at = tile(n)
        own_part[:, at] = x_ref[:, at].astype(F32) + dot(unpacked[0], w_out[:, at])
        return carry

    lax.fori_loop(0, 2 * per_half, own_step, 0)

    for k in range(4):
        partner_ahead(k).wait_send()
    out_ref = partner_x

    def finish(at):
        out_ref[:, at] = (own_part[:, at] + from_behind[:, at].astype(F32) + from_ahead[:, at].astype(F32)).astype(BF16)

    quarters = (
        (one, ("second_one", "first_low")),
        (two, ("second_two",)),
        (third, ("first_third", "second_third")),
        (fourth, ("first_fourth", "second_fourth")),
    )
    stores = [pltpu.make_async_copy(out_ref.at[:, at], out_hbm.at[:, at], out_sem.at[i]) for i, (at, _) in enumerate(quarters)]
    for i in range(4):
        at, names = quarters[i]
        for name in names:
            sums[name]().wait_recv()
        finish(at)
        stores[i].start()

    for k in range(4):
        own_ahead(k).wait_send()
        to_partner(k).wait_send()
        forward(k).wait_send()
    for c in range(4):
        all_but_one(sent, c, all_lanes if c < far else pair_lanes, send_sem.at[c])
        all_but_one(back_sent, c, query_lanes, back_send.at[c])
    all_but_one(sent, far, query_lanes, send_sem.at[4])
    for copy in sums.values():
        copy().wait_send()
    for copy in stores:
        copy.wait()


def body(tokens, norm_gain, w_query, w_key, w_value, w_output, doc_lengths, pack_index):
    groups = lax.axis_size("dp")
    members = lax.axis_size("tp")
    rows, width = tokens.shape
    piece = width // 4
    q_cols, k_cols = w_query.shape[1], w_key.shape[1]
    total_cols = q_cols + 2 * k_cols
    per_kv = q_cols // k_cols
    side = (per_kv + 2) * HEAD_DIM
    ctx = per_kv * HEAD_DIM
    chunk_slots = SLOTS * groups
    index = pack_index.reshape(groups * members, rows)
    hbm = pl.BlockSpec(memory_space=pl.ANY)
    dma = pltpu.SemaphoreType.DMA
    V = pltpu.VMEM
    return pl.pallas_call(
        kernel,
        out_shape=jax.ShapeDtypeStruct((rows, width), BF16),
        in_specs=[hbm] * 8,
        out_specs=hbm,
        scratch_shapes=[
            V((rows, width), BF16),
            V((1, width), F32),
            V((groups * members, rows), jnp.int32),
            V((1, doc_lengths.shape[0]), jnp.int32),
            V((rows, width), BF16),
            V((width, total_cols), BF16),
            V(w_output.shape, BF16),
            V((3, rows, width), BF16),
            V((2, rows, piece), BF16),
            V((4, rows, total_cols), F32),
            V((4, rows, 128), F32),
            V((2 * rows, side), BF16),
            V((4, rows, HEAD_DIM), F32),
            V((4, rows, HEAD_DIM), F32),
            V((4, 2 * SLOTS * groups, 2 * rows), BF16),
            V((4 * groups, 2 * SLOTS, side), BF16),
            V((4 * groups, 2 * SLOTS, side), BF16),
            V((2, 4 * chunk_slots, side + HEAD_DIM), BF16),
            V((1, 4 * chunk_slots), F32),
            V((4, chunk_slots, 128), F32),
            V((4, chunk_slots, 128), F32),
            V((chunk_slots, 4 * chunk_slots), F32),
            V((4, 2 * rows, 2 * SLOTS * groups), BF16),
            V((2, chunk_slots, ctx), BF16),
            V((4 * groups, 2 * SLOTS, ctx), BF16),
            V((4 * groups, 2 * SLOTS, ctx), BF16),
            V((4, rows, 2 * ctx), BF16),
            V((3, rows, width), BF16),
            V((rows, width // 2), BF16),
            V((rows, width // 2), BF16),
            V((rows, width), BF16),
            V((rows, width), BF16),
            V((rows, width), F32),
            V((q_cols // HEAD_DIM, chunk_slots, 2 * HEAD_DIM), F32),
            V((q_cols // HEAD_DIM, chunk_slots, HEAD_DIM), F32),
            dma((4,)),
            dma((4,)),
            dma((3, 4)),
            dma,
            dma((4,)),
            dma((4,)),
            dma((3, 4)),
            dma((3, 4)),
            dma((5,)),
            dma((5,)),
            dma((4,)),
            dma((4,)),
            dma((9,)),
            dma((9,)),
        ],
        compiler_params=pltpu.CompilerParams(
            collective_id=0, has_side_effects=True, vmem_limit_bytes=67043328
        ),
        name="packed_attention",
    )(tokens, norm_gain.reshape(1, width), index, doc_lengths.reshape(1, -1), w_query, w_key, w_value, w_output)


def solution(mesh):
    placed = (
        P(("dp", "tp"), None),
        P(),
        P(None, "tp"),
        P(None, "tp"),
        P(None, "tp"),
        P("tp", None),
        P(),
        P(),
    )
    return jax.shard_map(
        body, mesh=mesh, in_specs=placed, out_specs=P(("dp", "tp"), None), check_vma=False
    )
```

```python
import functools
import math

import jax
import jax.numpy as jnp
from jax import lax
from jax.experimental import pallas as pl
from jax.experimental.pallas import tpu as pltpu
from jax.sharding import PartitionSpec as P

HEAD_DIM = 128
GROUP_DOCS = 4
SLOTS = 8
rope_base = 500000.0
norm_eps = 1e-05
score_floor = -1e30
MESH = pl.DeviceIdType.MESH
F32 = jnp.float32
BF16 = jnp.bfloat16


def iota(shape, dim):
    return lax.broadcasted_iota(jnp.int32, shape, dim)


def kernel(
    x_hbm, gain_hbm, pidx_hbm, len_hbm, wq_ref, wk_ref, wv_ref, wo_ref,
    out_hbm,
    x_ref, gain_ref, pidx_ref, len_ref, partner_x,
    w_all, w_out, gathered, scaled, acc, sumsq, stacked, cosines, sines, picks, sent, arrived, qkv,
    slot_row, slot_col, slot_start, bias, unpack, mixed, back_sent, back, unpacked,
    part, half_a, half_b, from_behind, from_ahead, own_part, early, early_peak,
    in_sem, out_sem, w_sem, wo_sem, pair_send, pair_recv, ag_send, ag_recv,
    send_sem, recv_sem, back_send, back_recv, rs_send, rs_recv,
):
    groups = lax.axis_size("dp")
    rows, width = x_ref.shape
    piece = width // 4
    half = width // 2
    docs = len_ref.shape[1]
    me = lax.axis_index("dp")
    z = lax.axis_index("tp")
    right = lax.rem(z + 1, 4)
    left = lax.rem(z + 3, 4)
    core = lax.rem(me, 2)
    partner = me + 1 - 2 * core
    ahead = lax.rem(z + 1 + 2 * core, 4)
    behind = lax.rem(z + 3 - 2 * core, 4)
    own, first, far, second = 0, 1, 2, 3

    def member(c, parity):
        return lax.rem(z + (0, 3 - 2 * parity, 2, 1 + 2 * parity)[c], 4)

    q_cols = wq_ref.shape[1]
    k_cols = wk_ref.shape[1]
    heads = q_cols // HEAD_DIM
    kv_heads = k_cols // HEAD_DIM
    per_kv = heads // kv_heads
    side = (per_kv + 2) * HEAD_DIM
    ctx = per_kv * HEAD_DIM
    pack_rows = 2 * SLOTS
    stride = 11
    nb = min(16, groups)
    chunk_slots = SLOTS * groups

    def cols(k):
        return pl.ds(k * piece, piece) if isinstance(k, int) else pl.ds(pl.multiple_of(k * piece, 128), piece)

    def w_copies(k):
        at = cols(k)
        return (
            pltpu.make_async_copy(wq_ref.at[at, :], w_all.at[at, pl.ds(0, q_cols)], w_sem.at[0, k]),
            pltpu.make_async_copy(wk_ref.at[at, :], w_all.at[at, pl.ds(q_cols, k_cols)], w_sem.at[1, k]),
            pltpu.make_async_copy(wv_ref.at[at, :], w_all.at[at, pl.ds(q_cols + k_cols, k_cols)], w_sem.at[2, k]),
        )

    loads = [
        pltpu.make_async_copy(src, dst, in_sem.at[i])
        for i, (src, dst) in enumerate(
            ((x_hbm, x_ref), (gain_hbm, gain_ref), (pidx_hbm, pidx_ref), (len_hbm, len_ref))
        )
    ]
    for copy in loads:
        copy.start()
    wo_copy = pltpu.make_async_copy(wo_ref, w_out, wo_sem)

    barrier = pltpu.get_barrier_semaphore()

    def greet(i, carry):
        pl.semaphore_signal(barrier, inc=1, device_id=(lax.rem(me + i, groups), z), device_id_type=MESH)
        return carry

    for device in ((me, right), (me, left), (partner, ahead)):
        pl.semaphore_signal(barrier, inc=1, device_id=device, device_id_type=MESH)
    lax.fori_loop(1, groups, greet, 0)
    for copy in loads:
        copy.wait()
    for k in range(4):
        for copy in w_copies(k):
            copy.start()
    pl.semaphore_wait(barrier, groups + 2)

    def copy_to(src, dst, send, recv, device):
        return pltpu.make_async_remote_copy(
            src_ref=src, dst_ref=dst, send_sem=send, recv_sem=recv, device_id=device, device_id_type=MESH
        )

    def column_copy(src, dst, send, recv, to):
        return copy_to(src, dst, send, recv, (me, to))

    def own_ahead(k):
        return copy_to(
            x_ref.at[:, cols(k)], gathered.at[0, :, cols(k)], ag_send.at[0, k], ag_recv.at[0, k], (me, ahead)
        )

    def to_partner(k):
        return copy_to(x_ref.at[:, cols(k)], partner_x.at[:, cols(k)], pair_send.at[k], pair_recv.at[k], (partner, z))

    def partner_ahead(k):
        return copy_to(
            partner_x.at[:, cols(k)], gathered.at[2, :, cols(k)], ag_send.at[2, k], ag_recv.at[2, k], (partner, ahead)
        )

    def landed(c, k):
        piece_ref = gathered.at[c - 1, :, cols(k)]
        pltpu.make_async_copy(piece_ref, piece_ref, ag_recv.at[c - 1, k]).wait()

    def forward(k):
        return copy_to(
            gathered.at[0, :, cols(k)], gathered.at[1, :, cols(k)], ag_send.at[1, k], ag_recv.at[1, k], (me, ahead)
        )

    for k in range(4):
        own_ahead(k).start()
        to_partner(k).start()

    lane = iota((1, docs), 1)
    lens_row = len_ref[...].astype(F32)
    eye_docs = iota((docs, docs), 0) == iota((docs, docs), 1)
    lens_col = jnp.sum(jnp.where(eye_docs, lens_row, 0.0), axis=1, keepdims=True)
    before = iota((docs, docs), 0) < iota((docs, docs), 1)
    starts_row = jnp.sum(jnp.where(before, lens_col, 0.0), axis=0, keepdims=True)
    group_of = iota((groups, docs), 0)
    lane_g = iota((groups, docs), 1)
    group_lo = jnp.sum(jnp.where(lane_g < GROUP_DOCS * group_of, lens_row, 0.0), axis=1, keepdims=True)
    group_hi = jnp.sum(jnp.where(lane_g < GROUP_DOCS * (group_of + 1), lens_row, 0.0), axis=1, keepdims=True)

    def upto(count):
        return jnp.sum(jnp.where(lane < count, lens_row, 0.0), axis=1, keepdims=True)

    my_lo = upto(GROUP_DOCS * me)
    my_hi = upto(GROUP_DOCS * (me + 1))
    my_starts = [upto(GROUP_DOCS * me + i) - my_lo for i in range(1, GROUP_DOCS)]
    earlier = (iota((rows, rows), 0) < iota((rows, rows), 1)).astype(BF16)
    spread_p = (iota((pack_rows * groups, groups), 0) // pack_rows == iota((pack_rows * groups, groups), 1)).astype(BF16)
    spread_s = (iota((chunk_slots, groups), 0) // SLOTS == iota((chunk_slots, groups), 1)).astype(BF16)

    def dot(a, b):
        return jnp.dot(a, b, preferred_element_type=F32)

    def slot_tables(c):
        index = pidx_ref[pl.ds(member(c, 0), groups, stride=4), :]
        if c in (first, second):
            odd = iota((groups, rows), 0) % 2 == 1
            index = jnp.where(odd, pidx_ref[pl.ds(member(c, 1), groups, stride=4), :], index)
        index = index.astype(F32)
        mine = (index >= my_lo) & (index < my_hi)
        rank = dot(jnp.where(mine, 1.0, 0.0).astype(BF16), earlier)
        code = jnp.where(mine, rank, -1.0).astype(BF16)
        place = jnp.where(mine, index - my_lo, 0.0)
        high = jnp.floor(place * (1.0 / 32.0))
        low = place - high * 32.0
        code_s = dot(spread_s, code)
        place_s = dot(spread_s, high.astype(BF16)) * 32.0 + dot(spread_s, low.astype(BF16))
        wanted = (iota((chunk_slots, rows), 0) % SLOTS).astype(F32)
        found = jnp.sum(jnp.where(code_s == wanted, place_s + 1.0, 0.0), axis=1, keepdims=True) - 1.0
        begin = jnp.zeros_like(found)
        for start in my_starts:
            begin = jnp.where(found >= start, start, begin)
        slot_col[c] = jnp.broadcast_to(found, (chunk_slots, 128))
        slot_start[c] = jnp.broadcast_to(begin, (chunk_slots, 128))
        same = iota((chunk_slots, chunk_slots), 0) == iota((chunk_slots, chunk_slots), 1)
        slot_row[:, pl.ds(c * chunk_slots, chunk_slots)] = jnp.sum(jnp.where(same, found, 0.0), axis=0, keepdims=True)

    sumsq[...] = jnp.zeros_like(sumsq)
    acc[...] = jnp.zeros_like(acc)
    total_cols = q_cols + 2 * k_cols
    n_tile = 512

    n_tiles = total_cols // n_tile

    def scale_piece(c, k, slot, x):
        x = x.astype(F32)
        squares = sumsq[c]
        for j in range(piece // 128):
            block = x[:, j * 128 : (j + 1) * 128]
            squares = squares + block * block
        sumsq[c] = squares
        scaled[slot] = (x * gain_ref[:, cols(k)]).astype(BF16)

    def multiply(c, k, slot, tiles):
        for n in tiles:
            to = pl.ds(n * n_tile, n_tile)
            acc[c, :, to] += dot(scaled[slot], w_all[cols(k), to])

    def project(c, k, x):
        scale_piece(c, k, 0, x)
        multiply(c, k, 0, range(n_tiles))

    def prepare(c):
        index = pidx_ref[pl.ds(4 * me + member(c, core), 1), :].astype(F32)
        eye = iota((rows, rows), 0) == iota((rows, rows), 1)
        index_col = jnp.sum(jnp.where(eye, index, 0.0), axis=1, keepdims=True)
        begin = jnp.max(jnp.where(starts_row <= index_col, starts_row, 0.0), axis=1, keepdims=True)
        place = index_col - begin
        lanes = iota((1, HEAD_DIM), 1)
        exponent = (lanes % (HEAD_DIM // 2)).astype(F32) * (-2.0 * math.log(rope_base) / HEAD_DIM)
        angle = place * jnp.exp(exponent)
        cosines[c] = jnp.cos(angle)
        sines[c] = jnp.where(lanes < HEAD_DIM // 2, -1.0, 1.0) * jnp.sin(angle)
        inside = (index >= group_lo) & (index < group_hi)
        rank = dot(jnp.where(inside, 1.0, 0.0).astype(BF16), earlier)
        code = jnp.where(inside, rank, -100.0).astype(BF16)
        spread = dot(spread_p, code)
        wanted = (iota((pack_rows * groups, rows), 0) % pack_rows).astype(F32)
        for g in range(2):
            pick = jnp.where(spread + float(SLOTS * g) == wanted, 1.0, 0.0)
            unpack[c, pl.ds(g * rows, rows), :] = jnp.transpose(pick).astype(BF16)
            picks[c, :, pl.ds(g * rows, rows)] = pick.astype(BF16)

    query_lanes = pl.ds(0, ctx)
    pair_lanes = pl.ds(ctx, 2 * HEAD_DIM)
    all_lanes = pl.ds(0, side)

    def rotate_pairs(c, kind):
        scale = lax.rsqrt(jnp.sum(sumsq[c], axis=1, keepdims=True) * (1.0 / width) + norm_eps)
        cosine = cosines[c]
        sine = sines[c]
        query_scale = scale * (HEAD_DIM ** (-0.5) / math.log(2.0))

        def head(column, by):
            return acc[c, :, pl.ds(column * HEAD_DIM, HEAD_DIM)] * by

        def rope(t):
            return t * cosine + pltpu.roll(t, HEAD_DIM // 2, 1) * sine

        for g in range(kv_heads):
            at = pl.ds(g * rows, rows)
            if kind != "pair":
                for j in range(per_kv):
                    stacked[at, pl.ds(j * HEAD_DIM, HEAD_DIM)] = rope(head(g * per_kv + j, query_scale)).astype(BF16)
            if kind != "query":
                stacked[at, pl.ds(ctx, HEAD_DIM)] = rope(head(heads + g, scale)).astype(BF16)
                stacked[at, pl.ds(ctx + HEAD_DIM, HEAD_DIM)] = head(heads + kv_heads + g, scale).astype(BF16)

    def dispatch(c, kind="all"):
        lanes, sem = {"all": (all_lanes, c), "pair": (pair_lanes, c), "query": (query_lanes, 4)}[kind]
        rotate_pairs(c, kind)
        for b in range(groups // nb):
            block = picks[c, pl.ds(b * nb * pack_rows, nb * pack_rows), :]
            packed = dot(block, stacked[:, lanes]).astype(BF16)
            sent[pl.ds(c * groups + b * nb, nb), :, lanes] = packed.reshape(nb, pack_rows, packed.shape[1])
        arrived[c * groups + me, :, lanes] = sent[c * groups + me, :, lanes]

        def send(i, carry):
            to = lax.rem(me + stride * i, groups)
            pltpu.make_async_remote_copy(
                src_ref=sent.at[c * groups + to, :, lanes],
                dst_ref=arrived.at[c * groups + me, :, lanes],
                send_sem=send_sem.at[sem],
                recv_sem=recv_sem.at[sem],
                device_id=(to, z),
                device_id_type=MESH,
            ).start()
            return carry

        lax.fori_loop(1, groups, send, 0)

    def all_but_one(ref, c, lanes, sem):
        block = ref.at[pl.ds(c * groups, groups - 1), :, lanes]
        pltpu.make_async_copy(block, block, sem).wait()

    reorder_rows = pack_rows * nb
    out_row = iota((reorder_rows, reorder_rows), 0)
    in_row = iota((reorder_rows, reorder_rows), 1)
    split = nb * SLOTS
    source_row = (out_row % split) // SLOTS * pack_rows + out_row // split * SLOTS + out_row % SLOTS
    apart = (source_row == in_row).astype(BF16)
    source_back = (in_row % split) // SLOTS * pack_rows + in_row // split * SLOTS + in_row % SLOTS
    together = (source_back == out_row).astype(BF16)

    def receive(c, kind="all"):
        lanes, sem = {"all": (all_lanes, c), "pair": (pair_lanes, c), "query": (query_lanes, 4)}[kind]
        all_but_one(arrived, c, lanes, recv_sem.at[sem])
        for b in range(groups // nb):
            block = arrived[pl.ds(c * groups + b * nb, nb), :, lanes]
            ordered = dot(apart, block.reshape(reorder_rows, block.shape[2])).astype(BF16)
            for g in range(2):
                qkv[g, pl.ds(c * chunk_slots + b * split, split), lanes] = ordered[g * split : (g + 1) * split]

    def mask(c):
        found = slot_col[c][:, :1]
        begin = slot_start[c][:, :1]
        keys = slot_row[...]
        bias[...] = jnp.where((keys >= begin) & (keys <= found), 0.0, score_floor)

    early_keys = pl.ds(0, second * chunk_slots)
    late_keys = pl.ds(second * chunk_slots, chunk_slots)
    every_key = pl.ds(0, 4 * chunk_slots)

    def scored(c, i, keys):
        g = i // per_kv
        query = qkv[g, pl.ds(c * chunk_slots, chunk_slots), pl.ds(i % per_kv * HEAD_DIM, HEAD_DIM)]
        key = qkv[g, keys, pl.ds(ctx, HEAD_DIM)]
        scores = lax.dot_general(query, key, (((1,), (1,)), ((), ())), preferred_element_type=F32)
        scores = scores + bias[:, keys]
        return scores, jnp.max(scores, axis=1, keepdims=True)

    def weighted(i, scores, peak, keys):
        weights = jnp.exp2(scores - peak).astype(BF16)
        return dot(weights, qkv[i // per_kv, keys, pl.ds(ctx + HEAD_DIM, 2 * HEAD_DIM)])

    def attend_early(c):
        for i in range(heads):
            scores, peak = scored(c, i, early_keys)
            early[i] = weighted(i, scores, peak, early_keys)
            early_peak[i] = jnp.broadcast_to(peak, (chunk_slots, HEAD_DIM))

    def attend(c, resumed=False):
        for i in range(heads):
            keys = late_keys if resumed else every_key
            scores, peak = scored(c, i, keys)
            if resumed:
                before = early_peak[i][:, :1]
                peak = jnp.maximum(peak, before)
                both = early[i] * jnp.exp2(before - peak) + weighted(i, scores, peak, keys)
            else:
                both = weighted(i, scores, peak, keys)
            mixed[i // per_kv, :, pl.ds(i % per_kv * HEAD_DIM, HEAD_DIM)] = (
                both[:, :HEAD_DIM] / both[:, HEAD_DIM:]
            ).astype(BF16)
        for b in range(groups // nb):
            block = mixed[:, pl.ds(b * split, split), :].reshape(reorder_rows, ctx)
            back_sent[pl.ds(c * groups + b * nb, nb)] = dot(together, block).astype(BF16).reshape(nb, pack_rows, ctx)
        back[c * groups + me] = back_sent[c * groups + me]

        def send(i, carry):
            to = lax.rem(me + stride * i, groups)
            pltpu.make_async_remote_copy(
                src_ref=back_sent.at[c * groups + to],
                dst_ref=back.at[c * groups + me],
                send_sem=back_send.at[c],
                recv_sem=back_recv.at[c],
                device_id=(to, z),
                device_id_type=MESH,
            ).start()
            return carry

        lax.fori_loop(1, groups, send, 0)

    quarter = width // 4
    o_tile = min(512, quarter)
    per_quarter = quarter // o_tile

    def fetch(c):
        all_but_one(back, c, query_lanes, back_recv.at[c])
        block = back[pl.ds(c * groups, groups)].reshape(pack_rows * groups, ctx)
        both = dot(unpack[c], block).astype(BF16)
        for g in range(2):
            unpacked[c, :, pl.ds(g * ctx, ctx)] = both[g * rows : (g + 1) * rows]

    def tile(n):
        return pl.ds(pl.multiple_of(n * o_tile, 128), o_tile)

    def quarter_of(i):
        return pl.ds(i * quarter, quarter)

    def output_quarter(c, i, extra=None):
        for n in range(per_quarter):
            at = pl.ds(i * quarter + n * o_tile, o_tile)
            value = dot(unpacked[c], w_out[:, at])
            if extra is not None:
                value = value + extra[:, pl.ds(i % 2 * quarter + n * o_tile, o_tile)].astype(F32)
            part[c - 1, :, at] = value.astype(BF16)

    def partial_sum(c, i):
        at = quarter_of(i)
        if c == far:
            target, to = ((half_a, ahead), (half_b, behind))[i // 2]
            place = quarter_of(i % 2)
        else:
            target, to = ((from_behind, ahead) if c == second else (from_ahead, behind))
            place = at
        return column_copy(
            part.at[c - 1, :, at], target.at[:, place], rs_send.at[c - 1, i], rs_recv.at[c - 1, i], to
        )

    def output_send(c, i, extra=None):
        output_quarter(c, i, extra)
        partial_sum(c, i).start()

    for k in range(4):
        for copy in w_copies(k):
            copy.wait()
        project(0, k, x_ref[:, cols(k)])
    wo_copy.start()
    prepare(0)
    dispatch(0)
    for c in range(1, 4):
        prepare(c)
    for c in range(4):
        slot_tables(c)
    for g in range(2):
        qkv[g, :, pl.ds(side, HEAD_DIM)] = jnp.ones((4 * chunk_slots, HEAD_DIM), BF16)
    mask(far)

    for k in range(4):
        landed(first, k)
        forward(k).start()
        project(first, k, gathered[0, :, cols(k)])
    for k in range(4):
        to_partner(k).wait_recv()
        partner_ahead(k).start()
    dispatch(first)
    receive(own)

    def far_piece(k, carry):
        landed(far, k)
        project(far, k, gathered[1, :, cols(k)])
        return carry

    lax.fori_loop(0, 4, far_piece, 0)
    dispatch(far)
    receive(first)

    def second_piece(k, carry):
        landed(second, k)
        project(second, k, gathered[2, :, cols(k)])
        return carry

    lax.fori_loop(0, 3, second_piece, 0)
    landed(second, 3)
    scale_piece(second, 3, 0, gathered[2, :, cols(3)])
    multiply(second, 3, 0, range(n_tiles - 1, n_tiles))
    dispatch(second, "pair")
    multiply(second, 3, 0, range(n_tiles - 1))
    dispatch(second, "query")
    receive(far)
    attend_early(far)
    receive(second, "pair")
    attend(far, True)
    mask(first)
    attend(first)
    receive(second, "query")
    mask(second)
    attend(second)
    wo_copy.wait()
    fetch(far)
    for i in (0, 2, 1, 3):
        output_send(far, i)
    fetch(first)
    for i in (0, 1):
        output_send(first, i)
    mask(own)
    attend(own)
    fetch(second)
    for i in (2, 3):
        output_send(second, i)
    for i in (0, 1):
        partial_sum(far, i).wait_recv()
        output_send(second, i, half_a)
        partial_sum(far, i + 2).wait_recv()
        output_send(first, i + 2, half_b)
    fetch(own)

    def own_step(n, carry):
        at = pl.ds(pl.multiple_of(n * o_tile, 128), o_tile)
        own_part[:, at] = x_ref[:, at].astype(F32) + dot(unpacked[own], w_out[:, at])
        return carry

    lax.fori_loop(0, 4 * per_quarter, own_step, 0)
    for k in range(4):
        partner_ahead(k).wait_send()
    out_ref = partner_x

    def store(i):
        at = quarter_of(i)
        return pltpu.make_async_copy(out_ref.at[:, at], out_hbm.at[:, at], out_sem.at[i])

    for i in (0, 2, 1, 3):
        at = quarter_of(i)
        partial_sum(second, i).wait_recv()
        partial_sum(first, i).wait_recv()
        out_ref[:, at] = (own_part[:, at] + from_behind[:, at].astype(F32) + from_ahead[:, at].astype(F32)).astype(BF16)
        store(i).start()

    for k in range(4):
        own_ahead(k).wait_send()
        to_partner(k).wait_send()
        forward(k).wait_send()
    for c in range(4):
        all_but_one(sent, c, all_lanes if c < second else pair_lanes, send_sem.at[c])
        all_but_one(back_sent, c, query_lanes, back_send.at[c])
    all_but_one(sent, second, query_lanes, send_sem.at[4])
    for c in (first, far, second):
        for i in range(4):
            partial_sum(c, i).wait_send()
    for i in range(4):
        store(i).wait()


def body(tokens, norm_gain, w_query, w_key, w_value, w_output, doc_lengths, pack_index):
    groups = lax.axis_size("dp")
    members = lax.axis_size("tp")
    rows, width = tokens.shape
    piece = width // 4
    q_cols, k_cols = w_query.shape[1], w_key.shape[1]
    total_cols = q_cols + 2 * k_cols
    per_kv = q_cols // k_cols
    side = (per_kv + 2) * HEAD_DIM
    ctx = per_kv * HEAD_DIM
    chunk_slots = SLOTS * groups
    index = pack_index.reshape(groups * members, rows)
    hbm = pl.BlockSpec(memory_space=pl.ANY)
    dma = pltpu.SemaphoreType.DMA
    V = pltpu.VMEM
    return pl.pallas_call(
        kernel,
        out_shape=jax.ShapeDtypeStruct((rows, width), BF16),
        in_specs=[hbm] * 8,
        out_specs=hbm,
        scratch_shapes=[
            V((rows, width), BF16),
            V((1, width), F32),
            V((groups * members, rows), jnp.int32),
            V((1, doc_lengths.shape[0]), jnp.int32),
            V((rows, width), BF16),
            V((width, total_cols), BF16),
            V(w_output.shape, BF16),
            V((3, rows, width), BF16),
            V((1, rows, piece), BF16),
            V((4, rows, total_cols), F32),
            V((4, rows, 128), F32),
            V((2 * rows, side), BF16),
            V((4, rows, HEAD_DIM), F32),
            V((4, rows, HEAD_DIM), F32),
            V((4, 2 * SLOTS * groups, 2 * rows), BF16),
            V((4 * groups, 2 * SLOTS, side), BF16),
            V((4 * groups, 2 * SLOTS, side), BF16),
            V((2, 4 * chunk_slots, side + HEAD_DIM), BF16),
            V((1, 4 * chunk_slots), F32),
            V((4, chunk_slots, 128), F32),
            V((4, chunk_slots, 128), F32),
            V((chunk_slots, 4 * chunk_slots), F32),
            V((4, 2 * rows, 2 * SLOTS * groups), BF16),
            V((2, chunk_slots, ctx), BF16),
            V((4 * groups, 2 * SLOTS, ctx), BF16),
            V((4 * groups, 2 * SLOTS, ctx), BF16),
            V((4, rows, 2 * ctx), BF16),
            V((3, rows, width), BF16),
            V((rows, width // 2), BF16),
            V((rows, width // 2), BF16),
            V((rows, width), BF16),
            V((rows, width), BF16),
            V((rows, width), F32),
            V((q_cols // HEAD_DIM, chunk_slots, 2 * HEAD_DIM), F32),
            V((q_cols // HEAD_DIM, chunk_slots, HEAD_DIM), F32),
            dma((4,)),
            dma((4,)),
            dma((3, 4)),
            dma,
            dma((4,)),
            dma((4,)),
            dma((3, 4)),
            dma((3, 4)),
            dma((5,)),
            dma((5,)),
            dma((4,)),
            dma((4,)),
            dma((3, 4)),
            dma((3, 4)),
        ],
        compiler_params=pltpu.CompilerParams(
            collective_id=0, has_side_effects=True, vmem_limit_bytes=67043328
        ),
        name="packed_attention",
    )(tokens, norm_gain.reshape(1, width), index, doc_lengths.reshape(1, -1), w_query, w_key, w_value, w_output)


def solution(mesh):
    placed = (
        P(("dp", "tp"), None),
        P(),
        P(None, "tp"),
        P(None, "tp"),
        P(None, "tp"),
        P("tp", None),
        P(),
        P(),
    )
    return jax.shard_map(
        body, mesh=mesh, in_specs=placed, out_specs=P(("dp", "tp"), None), check_vma=False
    )
```

```python
import functools
import math

import jax
import jax.numpy as jnp
from jax import lax
from jax.experimental import pallas as pl
from jax.experimental.pallas import tpu as pltpu
from jax.sharding import PartitionSpec as P

HEAD_DIM = 128
GROUP_DOCS = 4
SLOTS = 8
rope_base = 500000.0
norm_eps = 1e-05
score_floor = -1e30
MESH = pl.DeviceIdType.MESH
F32 = jnp.float32
BF16 = jnp.bfloat16


def iota(shape, dim):
    return lax.broadcasted_iota(jnp.int32, shape, dim)


def kernel(
    x_hbm, gain_hbm, pidx_hbm, len_hbm, wq_ref, wk_ref, wv_ref, wo_ref,
    out_hbm,
    x_ref, gain_ref, pidx_ref, len_ref, partner_x,
    w_all, w_out, gathered, scaled, acc, sumsq, stacked, cosines, sines, picks, sent, arrived,
    sent_pair, arrived_pair, sent_query, arrived_query, qkv,
    slot_row, slot_col, slot_start, bias, unpack, mixed, back_sent, back, far_sent, far_back, unpacked,
    part, half_a, half_b, from_behind, from_ahead, own_part, early, early_peak,
    in_sem, out_sem, w_sem, wo_sem, pair_send, pair_recv, ag_send, ag_recv,
    send_sem, recv_sem, back_send, back_recv, rs_send, rs_recv,
):
    groups = lax.axis_size("dp")
    rows, width = x_ref.shape
    piece = width // 4
    half = width // 2
    docs = len_ref.shape[1]
    me = lax.axis_index("dp")
    z = lax.axis_index("tp")
    right = lax.rem(z + 1, 4)
    left = lax.rem(z + 3, 4)
    core = lax.rem(me, 2)
    partner = me + 1 - 2 * core
    ahead = lax.rem(z + 1 + 2 * core, 4)
    behind = lax.rem(z + 3 - 2 * core, 4)
    own, first, far, second = 0, 1, 2, 3

    def member(c, parity):
        return lax.rem(z + (0, 3 - 2 * parity, 2, 1 + 2 * parity)[c], 4)

    q_cols = wq_ref.shape[1]
    k_cols = wk_ref.shape[1]
    heads = q_cols // HEAD_DIM
    kv_heads = k_cols // HEAD_DIM
    per_kv = heads // kv_heads
    side = (per_kv + 2) * HEAD_DIM
    ctx = per_kv * HEAD_DIM
    pack_rows = 2 * SLOTS
    stride = 11
    nb = min(16, groups)
    chunk_slots = SLOTS * groups

    def cols(k):
        return pl.ds(k * piece, piece) if isinstance(k, int) else pl.ds(pl.multiple_of(k * piece, 128), piece)

    def w_copies(k):
        at = cols(k)
        return (
            pltpu.make_async_copy(wq_ref.at[at, :], w_all.at[at, pl.ds(0, q_cols)], w_sem.at[0, k]),
            pltpu.make_async_copy(wk_ref.at[at, :], w_all.at[at, pl.ds(q_cols, k_cols)], w_sem.at[1, k]),
            pltpu.make_async_copy(wv_ref.at[at, :], w_all.at[at, pl.ds(q_cols + k_cols, k_cols)], w_sem.at[2, k]),
        )

    loads = [
        pltpu.make_async_copy(src, dst, in_sem.at[i])
        for i, (src, dst) in enumerate(
            ((x_hbm, x_ref), (gain_hbm, gain_ref), (pidx_hbm, pidx_ref), (len_hbm, len_ref))
        )
    ]
    for copy in loads:
        copy.start()
    wo_copy = pltpu.make_async_copy(wo_ref, w_out, wo_sem)

    barrier = pltpu.get_barrier_semaphore()

    def greet(i, carry):
        pl.semaphore_signal(barrier, inc=1, device_id=(lax.rem(me + i, groups), z), device_id_type=MESH)
        return carry

    for device in ((me, right), (me, left), (partner, ahead)):
        pl.semaphore_signal(barrier, inc=1, device_id=device, device_id_type=MESH)
    lax.fori_loop(1, groups, greet, 0)
    for copy in loads:
        copy.wait()
    for k in range(4):
        for copy in w_copies(k):
            copy.start()
    pl.semaphore_wait(barrier, groups + 2)

    def copy_to(src, dst, send, recv, device):
        return pltpu.make_async_remote_copy(
            src_ref=src, dst_ref=dst, send_sem=send, recv_sem=recv, device_id=device, device_id_type=MESH
        )

    def column_copy(src, dst, send, recv, to):
        return copy_to(src, dst, send, recv, (me, to))

    def own_ahead(k):
        return copy_to(
            x_ref.at[:, cols(k)], gathered.at[0, :, cols(k)], ag_send.at[0, k], ag_recv.at[0, k], (me, ahead)
        )

    def to_partner(k):
        return copy_to(x_ref.at[:, cols(k)], partner_x.at[:, cols(k)], pair_send.at[k], pair_recv.at[k], (partner, z))

    def partner_ahead(k):
        return copy_to(
            partner_x.at[:, cols(k)], gathered.at[2, :, cols(k)], ag_send.at[2, k], ag_recv.at[2, k], (partner, ahead)
        )

    def landed(c, k):
        piece_ref = gathered.at[c - 1, :, cols(k)]
        pltpu.make_async_copy(piece_ref, piece_ref, ag_recv.at[c - 1, k]).wait()

    def forward(k):
        return copy_to(
            gathered.at[0, :, cols(k)], gathered.at[1, :, cols(k)], ag_send.at[1, k], ag_recv.at[1, k], (me, ahead)
        )

    for k in range(4):
        own_ahead(k).start()
        to_partner(k).start()

    lane = iota((1, docs), 1)
    lens_row = len_ref[...].astype(F32)
    eye_docs = iota((docs, docs), 0) == iota((docs, docs), 1)
    lens_col = jnp.sum(jnp.where(eye_docs, lens_row, 0.0), axis=1, keepdims=True)
    before = iota((docs, docs), 0) < iota((docs, docs), 1)
    starts_row = jnp.sum(jnp.where(before, lens_col, 0.0), axis=0, keepdims=True)
    group_of = iota((groups, docs), 0)
    lane_g = iota((groups, docs), 1)
    group_lo = jnp.sum(jnp.where(lane_g < GROUP_DOCS * group_of, lens_row, 0.0), axis=1, keepdims=True)
    group_hi = jnp.sum(jnp.where(lane_g < GROUP_DOCS * (group_of + 1), lens_row, 0.0), axis=1, keepdims=True)

    def upto(count):
        return jnp.sum(jnp.where(lane < count, lens_row, 0.0), axis=1, keepdims=True)

    my_lo = upto(GROUP_DOCS * me)
    my_hi = upto(GROUP_DOCS * (me + 1))
    my_starts = [upto(GROUP_DOCS * me + i) - my_lo for i in range(1, GROUP_DOCS)]
    earlier = (iota((rows, rows), 0) < iota((rows, rows), 1)).astype(BF16)
    spread_p = (iota((pack_rows * groups, groups), 0) // pack_rows == iota((pack_rows * groups, groups), 1)).astype(BF16)
    spread_s = (iota((chunk_slots, groups), 0) // SLOTS == iota((chunk_slots, groups), 1)).astype(BF16)

    def dot(a, b):
        return jnp.dot(a, b, preferred_element_type=F32)

    def slot_tables(c):
        index = pidx_ref[pl.ds(member(c, 0), groups, stride=4), :]
        if c in (first, second):
            odd = iota((groups, rows), 0) % 2 == 1
            index = jnp.where(odd, pidx_ref[pl.ds(member(c, 1), groups, stride=4), :], index)
        index = index.astype(F32)
        mine = (index >= my_lo) & (index < my_hi)
        rank = dot(jnp.where(mine, 1.0, 0.0).astype(BF16), earlier)
        code = jnp.where(mine, rank, -1.0).astype(BF16)
        place = jnp.where(mine, index - my_lo, 0.0)
        high = jnp.floor(place * (1.0 / 32.0))
        low = place - high * 32.0
        code_s = dot(spread_s, code)
        place_s = dot(spread_s, high.astype(BF16)) * 32.0 + dot(spread_s, low.astype(BF16))
        wanted = (iota((chunk_slots, rows), 0) % SLOTS).astype(F32)
        found = jnp.sum(jnp.where(code_s == wanted, place_s + 1.0, 0.0), axis=1, keepdims=True) - 1.0
        begin = jnp.zeros_like(found)
        for start in my_starts:
            begin = jnp.where(found >= start, start, begin)
        slot_col[c] = jnp.broadcast_to(found, (chunk_slots, 128))
        slot_start[c] = jnp.broadcast_to(begin, (chunk_slots, 128))
        same = iota((chunk_slots, chunk_slots), 0) == iota((chunk_slots, chunk_slots), 1)
        slot_row[:, pl.ds(c * chunk_slots, chunk_slots)] = jnp.sum(jnp.where(same, found, 0.0), axis=0, keepdims=True)

    sumsq[...] = jnp.zeros_like(sumsq)
    acc[...] = jnp.zeros_like(acc)
    total_cols = q_cols + 2 * k_cols
    n_tile = 512

    n_tiles = total_cols // n_tile

    def scale_piece(c, k, slot, x):
        x = x.astype(F32)
        squares = sumsq[c]
        for j in range(piece // 128):
            block = x[:, j * 128 : (j + 1) * 128]
            squares = squares + block * block
        sumsq[c] = squares
        scaled[slot] = (x * gain_ref[:, cols(k)]).astype(BF16)

    def multiply(c, k, slot, tiles):
        for n in tiles:
            to = pl.ds(n * n_tile, n_tile)
            acc[c, :, to] += dot(scaled[slot], w_all[cols(k), to])

    def project(c, k, x):
        scale_piece(c, k, 0, x)
        multiply(c, k, 0, range(n_tiles))

    def prepare(c):
        index = pidx_ref[pl.ds(4 * me + member(c, core), 1), :].astype(F32)
        eye = iota((rows, rows), 0) == iota((rows, rows), 1)
        index_col = jnp.sum(jnp.where(eye, index, 0.0), axis=1, keepdims=True)
        begin = jnp.max(jnp.where(starts_row <= index_col, starts_row, 0.0), axis=1, keepdims=True)
        place = index_col - begin
        lanes = iota((1, HEAD_DIM), 1)
        exponent = (lanes % (HEAD_DIM // 2)).astype(F32) * (-2.0 * math.log(rope_base) / HEAD_DIM)
        angle = place * jnp.exp(exponent)
        cosines[c] = jnp.cos(angle)
        sines[c] = jnp.where(lanes < HEAD_DIM // 2, -1.0, 1.0) * jnp.sin(angle)
        inside = (index >= group_lo) & (index < group_hi)
        rank = dot(jnp.where(inside, 1.0, 0.0).astype(BF16), earlier)
        code = jnp.where(inside, rank, -100.0).astype(BF16)
        spread = dot(spread_p, code)
        wanted = (iota((pack_rows * groups, rows), 0) % pack_rows).astype(F32)
        for g in range(2):
            pick = jnp.where(spread + float(SLOTS * g) == wanted, 1.0, 0.0)
            unpack[c, pl.ds(g * rows, rows), :] = jnp.transpose(pick).astype(BF16)
            picks[c, :, pl.ds(g * rows, rows)] = pick.astype(BF16)

    query_lanes = pl.ds(0, ctx)
    pair_lanes = pl.ds(ctx, 2 * HEAD_DIM)
    all_lanes = pl.ds(0, side)

    def rotate_pairs(c, kind):
        scale = lax.rsqrt(jnp.sum(sumsq[c], axis=1, keepdims=True) * (1.0 / width) + norm_eps)
        cosine = cosines[c]
        sine = sines[c]
        query_scale = scale * (HEAD_DIM ** (-0.5) / math.log(2.0))

        def head(column, by):
            return acc[c, :, pl.ds(column * HEAD_DIM, HEAD_DIM)] * by

        def rope(t):
            return t * cosine + pltpu.roll(t, HEAD_DIM // 2, 1) * sine

        for g in range(kv_heads):
            at = pl.ds(g * rows, rows)
            if kind != "pair":
                for j in range(per_kv):
                    stacked[at, pl.ds(j * HEAD_DIM, HEAD_DIM)] = rope(head(g * per_kv + j, query_scale)).astype(BF16)
            if kind != "query":
                stacked[at, pl.ds(ctx, HEAD_DIM)] = rope(head(heads + g, scale)).astype(BF16)
                stacked[at, pl.ds(ctx + HEAD_DIM, HEAD_DIM)] = head(heads + kv_heads + g, scale).astype(BF16)

    def wires(c, kind):
        if kind == "pair":
            return pair_lanes, sent_pair, arrived_pair, c
        if kind == "query":
            return query_lanes, sent_query, arrived_query, 4
        at = pl.ds(c * groups, groups)
        return all_lanes, sent.at[at], arrived.at[at], c

    def scatter(source, target, send_at, recv_at):
        def send(i, carry):
            to = lax.rem(me + stride * i, groups)
            pltpu.make_async_remote_copy(
                src_ref=source.at[to],
                dst_ref=target.at[me],
                send_sem=send_at,
                recv_sem=recv_at,
                device_id=(to, z),
                device_id_type=MESH,
            ).start()
            return carry

        lax.fori_loop(1, groups, send, 0)

    def dispatch(c, kind="all"):
        lanes, source, target, sem = wires(c, kind)
        rotate_pairs(c, kind)
        for b in range(groups // nb):
            block = picks[c, pl.ds(b * nb * pack_rows, nb * pack_rows), :]
            packed = dot(block, stacked[:, lanes]).astype(BF16)
            source[pl.ds(b * nb, nb)] = packed.reshape(nb, pack_rows, packed.shape[1])
        target[me] = source[me]
        scatter(source, target, send_sem.at[sem], recv_sem.at[sem])

    def all_but_one(ref, sem):
        block = ref.at[pl.ds(0, groups - 1)]
        pltpu.make_async_copy(block, block, sem).wait()

    reorder_rows = pack_rows * nb
    out_row = iota((reorder_rows, reorder_rows), 0)
    in_row = iota((reorder_rows, reorder_rows), 1)
    split = nb * SLOTS
    source_row = (out_row % split) // SLOTS * pack_rows + out_row // split * SLOTS + out_row % SLOTS
    apart = (source_row == in_row).astype(BF16)
    source_back = (in_row % split) // SLOTS * pack_rows + in_row // split * SLOTS + in_row % SLOTS
    together = (source_back == out_row).astype(BF16)

    def receive(c, kind="all"):
        lanes, _, target, sem = wires(c, kind)
        all_but_one(target, recv_sem.at[sem])
        for b in range(groups // nb):
            block = target[pl.ds(b * nb, nb)]
            ordered = dot(apart, block.reshape(reorder_rows, block.shape[2])).astype(BF16)
            for g in range(2):
                qkv[g, pl.ds(c * chunk_slots + b * split, split), lanes] = ordered[g * split : (g + 1) * split]

    def mask(c):
        found = slot_col[c][:, :1]
        begin = slot_start[c][:, :1]
        keys = slot_row[...]
        bias[...] = jnp.where((keys >= begin) & (keys <= found), 0.0, score_floor)

    early_keys = pl.ds(0, second * chunk_slots)
    late_keys = pl.ds(second * chunk_slots, chunk_slots)
    every_key = pl.ds(0, 4 * chunk_slots)

    def scored(c, i, keys):
        g = i // per_kv
        query = qkv[g, pl.ds(c * chunk_slots, chunk_slots), pl.ds(i % per_kv * HEAD_DIM, HEAD_DIM)]
        key = qkv[g, keys, pl.ds(ctx, HEAD_DIM)]
        scores = lax.dot_general(query, key, (((1,), (1,)), ((), ())), preferred_element_type=F32)
        scores = scores + bias[:, keys]
        return scores, jnp.max(scores, axis=1, keepdims=True)

    def weighted(i, scores, peak, keys):
        weights = jnp.exp2(scores - peak).astype(BF16)
        return dot(weights, qkv[i // per_kv, keys, pl.ds(ctx + HEAD_DIM, 2 * HEAD_DIM)])

    def attend_early(c):
        for i in range(heads):
            scores, peak = scored(c, i, early_keys)
            early[i] = weighted(i, scores, peak, early_keys)
            early_peak[i] = jnp.broadcast_to(peak, (chunk_slots, HEAD_DIM))

    share = ctx // 2

    def returns(c):
        if c == far:
            return [(pl.ds(i * share, share), far_sent.at[i], far_back.at[i], (c, 4)[i]) for i in range(2)]
        at = pl.ds((0, 1, None, 2)[c] * groups, groups)
        return [(query_lanes, back_sent.at[at], back.at[at], c)]

    def send_back(lanes, source, target, sem):
        for b in range(groups // nb):
            block = mixed[:, pl.ds(b * split, split), lanes]
            block = dot(together, block.reshape(reorder_rows, block.shape[2])).astype(BF16)
            source[pl.ds(b * nb, nb)] = block.reshape(nb, pack_rows, block.shape[1])
        target[me] = source[me]
        scatter(source, target, back_send.at[sem], back_recv.at[sem])

    def attend(c, resumed=False):
        wanted = returns(c)
        for j in range(per_kv):
            for g in range(kv_heads):
                i = g * per_kv + j
                keys = late_keys if resumed else every_key
                scores, peak = scored(c, i, keys)
                if resumed:
                    before = early_peak[i][:, :1]
                    peak = jnp.maximum(peak, before)
                    both = early[i] * jnp.exp2(before - peak) + weighted(i, scores, peak, keys)
                else:
                    both = weighted(i, scores, peak, keys)
                mixed[g, :, pl.ds(j * HEAD_DIM, HEAD_DIM)] = (both[:, :HEAD_DIM] / both[:, HEAD_DIM:]).astype(BF16)
            if (j + 1) * len(wanted) % per_kv == 0:
                send_back(*wanted[(j + 1) * len(wanted) // per_kv - 1])

    quarter = width // 4
    o_tile = min(512, quarter)
    per_quarter = quarter // o_tile

    def fetch(c):
        for lanes, _, target, sem in returns(c):
            all_but_one(target, back_recv.at[sem])
            block = target[...]
            both = dot(unpack[c], block.reshape(pack_rows * groups, block.shape[2])).astype(BF16)
            for g in range(2):
                at = pl.ds(g * ctx + lanes.start, lanes.size)
                unpacked[c, :, at] = both[g * rows : (g + 1) * rows]

    def quarter_of(i):
        return pl.ds(i * quarter, quarter)

    def output_quarter(c, i, extra=None):
        for n in range(per_quarter):
            at = pl.ds(i * quarter + n * o_tile, o_tile)
            value = dot(unpacked[c], w_out[:, at])
            if extra is not None:
                value = value + extra[:, pl.ds(i % 2 * quarter + n * o_tile, o_tile)].astype(F32)
            part[c - 1, :, at] = value.astype(BF16)

    def partial_sum(c, i):
        at = quarter_of(i)
        if c == far:
            target, to = ((half_a, ahead), (half_b, behind))[i // 2]
            place = quarter_of(i % 2)
        else:
            target, to = ((from_behind, ahead) if c == second else (from_ahead, behind))
            place = at
        return column_copy(
            part.at[c - 1, :, at], target.at[:, place], rs_send.at[c - 1, i], rs_recv.at[c - 1, i], to
        )

    def output_send(c, i, extra=None):
        output_quarter(c, i, extra)
        partial_sum(c, i).start()

    for k in range(4):
        for copy in w_copies(k):
            copy.wait()
        project(0, k, x_ref[:, cols(k)])
    wo_copy.start()
    prepare(0)
    dispatch(0)
    for c in range(1, 4):
        prepare(c)
    for c in range(4):
        slot_tables(c)
    for g in range(2):
        qkv[g, :, pl.ds(side, HEAD_DIM)] = jnp.ones((4 * chunk_slots, HEAD_DIM), BF16)
    mask(far)

    def first_piece(k, carry):
        landed(first, k)
        forward(k).start()
        project(first, k, gathered[0, :, cols(k)])
        return carry

    lax.fori_loop(0, 4, first_piece, 0)
    for k in range(4):
        to_partner(k).wait_recv()
        partner_ahead(k).start()
    dispatch(first)
    receive(own)

    def far_piece(k, carry):
        landed(far, k)
        project(far, k, gathered[1, :, cols(k)])
        return carry

    lax.fori_loop(0, 4, far_piece, 0)
    dispatch(far)
    receive(first)

    def second_piece(k, carry):
        landed(second, k)
        project(second, k, gathered[2, :, cols(k)])
        return carry

    lax.fori_loop(0, 3, second_piece, 0)
    landed(second, 3)
    scale_piece(second, 3, 0, gathered[2, :, cols(3)])
    multiply(second, 3, 0, range(n_tiles - 1, n_tiles))
    dispatch(second, "pair")
    multiply(second, 3, 0, range(n_tiles - 1))
    dispatch(second, "query")
    receive(far)
    attend_early(far)
    receive(second, "pair")
    attend(far, True)
    mask(first)
    attend(first)
    receive(second, "query")
    mask(second)
    wo_copy.wait()
    fetch(far)
    for i in (0, 2, 1, 3):
        output_send(far, i)
    attend(second)
    fetch(first)
    for i in (0, 1):
        output_send(first, i)
    mask(own)
    attend(own)
    fetch(second)
    for i in (2, 3):
        output_send(second, i)
    for i in (0, 1):
        partial_sum(far, i).wait_recv()
        output_send(second, i, half_a)
        partial_sum(far, i + 2).wait_recv()
        output_send(first, i + 2, half_b)
    fetch(own)

    def own_step(n, carry):
        at = pl.ds(pl.multiple_of(n * o_tile, 128), o_tile)
        own_part[:, at] = x_ref[:, at].astype(F32) + dot(unpacked[own], w_out[:, at])
        return carry

    lax.fori_loop(0, 4 * per_quarter, own_step, 0)
    for k in range(4):
        partner_ahead(k).wait_send()
    out_ref = partner_x

    def store(i):
        at = quarter_of(i)
        return pltpu.make_async_copy(out_ref.at[:, at], out_hbm.at[:, at], out_sem.at[i])

    for i in (0, 2, 1, 3):
        at = quarter_of(i)
        partial_sum(second, i).wait_recv()
        partial_sum(first, i).wait_recv()
        out_ref[:, at] = (own_part[:, at] + from_behind[:, at].astype(F32) + from_ahead[:, at].astype(F32)).astype(BF16)
        store(i).start()

    for k in range(4):
        own_ahead(k).wait_send()
        to_partner(k).wait_send()
        forward(k).wait_send()
    for c, kind in ((own, "all"), (first, "all"), (far, "all"), (second, "pair"), (second, "query")):
        _, source, _, sem = wires(c, kind)
        all_but_one(source, send_sem.at[sem])
    for c in range(4):
        for _, source, _, sem in returns(c):
            all_but_one(source, back_send.at[sem])
    for c in (first, far, second):
        for i in range(4):
            partial_sum(c, i).wait_send()
    for i in range(4):
        store(i).wait()


def body(tokens, norm_gain, w_query, w_key, w_value, w_output, doc_lengths, pack_index):
    groups = lax.axis_size("dp")
    members = lax.axis_size("tp")
    rows, width = tokens.shape
    piece = width // 4
    q_cols, k_cols = w_query.shape[1], w_key.shape[1]
    total_cols = q_cols + 2 * k_cols
    per_kv = q_cols // k_cols
    side = (per_kv + 2) * HEAD_DIM
    ctx = per_kv * HEAD_DIM
    chunk_slots = SLOTS * groups
    index = pack_index.reshape(groups * members, rows)
    hbm = pl.BlockSpec(memory_space=pl.ANY)
    dma = pltpu.SemaphoreType.DMA
    V = pltpu.VMEM
    return pl.pallas_call(
        kernel,
        out_shape=jax.ShapeDtypeStruct((rows, width), BF16),
        in_specs=[hbm] * 8,
        out_specs=hbm,
        scratch_shapes=[
            V((rows, width), BF16),
            V((1, width), F32),
            V((groups * members, rows), jnp.int32),
            V((1, doc_lengths.shape[0]), jnp.int32),
            V((rows, width), BF16),
            V((width, total_cols), BF16),
            V(w_output.shape, BF16),
            V((3, rows, width), BF16),
            V((1, rows, piece), BF16),
            V((4, rows, total_cols), F32),
            V((4, rows, 128), F32),
            V((2 * rows, side), BF16),
            V((4, rows, HEAD_DIM), F32),
            V((4, rows, HEAD_DIM), F32),
            V((4, 2 * SLOTS * groups, 2 * rows), BF16),
            V((3 * groups, 2 * SLOTS, side), BF16),
            V((3 * groups, 2 * SLOTS, side), BF16),
            V((groups, 2 * SLOTS, 2 * HEAD_DIM), BF16),
            V((groups, 2 * SLOTS, 2 * HEAD_DIM), BF16),
            V((groups, 2 * SLOTS, ctx), BF16),
            V((groups, 2 * SLOTS, ctx), BF16),
            V((2, 4 * chunk_slots, side + HEAD_DIM), BF16),
            V((1, 4 * chunk_slots), F32),
            V((4, chunk_slots, 128), F32),
            V((4, chunk_slots, 128), F32),
            V((chunk_slots, 4 * chunk_slots), F32),
            V((4, 2 * rows, 2 * SLOTS * groups), BF16),
            V((2, chunk_slots, ctx), BF16),
            V((3 * groups, 2 * SLOTS, ctx), BF16),
            V((3 * groups, 2 * SLOTS, ctx), BF16),
            V((2, groups, 2 * SLOTS, ctx // 2), BF16),
            V((2, groups, 2 * SLOTS, ctx // 2), BF16),
            V((4, rows, 2 * ctx), BF16),
            V((3, rows, width), BF16),
            V((rows, width // 2), BF16),
            V((rows, width // 2), BF16),
            V((rows, width), BF16),
            V((rows, width), BF16),
            V((rows, width), F32),
            V((q_cols // HEAD_DIM, chunk_slots, 2 * HEAD_DIM), F32),
            V((q_cols // HEAD_DIM, chunk_slots, HEAD_DIM), F32),
            dma((4,)),
            dma((4,)),
            dma((3, 4)),
            dma,
            dma((4,)),
            dma((4,)),
            dma((3, 4)),
            dma((3, 4)),
            dma((5,)),
            dma((5,)),
            dma((5,)),
            dma((5,)),
            dma((3, 4)),
            dma((3, 4)),
        ],
        compiler_params=pltpu.CompilerParams(
            collective_id=0, has_side_effects=True, vmem_limit_bytes=67043328
        ),
        name="packed_attention",
    )(tokens, norm_gain.reshape(1, width), index, doc_lengths.reshape(1, -1), w_query, w_key, w_value, w_output)


def solution(mesh):
    placed = (
        P(("dp", "tp"), None),
        P(),
        P(None, "tp"),
        P(None, "tp"),
        P(None, "tp"),
        P("tp", None),
        P(),
        P(),
    )
    return jax.shard_map(
        body, mesh=mesh, in_specs=placed, out_specs=P(("dp", "tp"), None), check_vma=False
    )
```
